256 devices in a mesh: seq: 64 (over y_hi, x, z), mp: 4 (over y_lo, core).
Axes of the slice: x: 4, y: 4 (y_hi: 2, y_lo: 2; y = y_hi * 2 + y_lo), z: 8, core: 2. Of those that a mesh axis runs over, the one named last changes fastest.
Arguments:
- tokens: bfloat16 [256, 3584], P('mp'), may hold values from -6 to 6
- gain_attn: float32 [3584], replicated, may hold values from 0.25 to 1.75
- w_query: bfloat16 [3584, 3584], P(None, 'seq'), may hold values from -0.09375 to 0.09375
- query_bias: float32 [3584], P('seq'), may hold values from -3 to 3
- cache_keys: bfloat16 [4, 65536, 128], P(None, 'seq'), may hold values from -80 to 80
- cache_values: bfloat16 [4, 65536, 128], P(None, 'seq'), may hold values from -6 to 6
- w_out: bfloat16 [3584, 3584], P(None, 'seq'), may hold values from -0.09375 to 0.09375
- gain_ffn: float32 [3584], P('seq'), may hold values from 0.25 to 1.75
- w_gate: bfloat16 [3584, 18944], P('mp', 'seq'), may hold values from -0.09375 to 0.09375
- w_up: bfloat16 [3584, 18944], P('mp', 'seq'), may hold values from -0.09375 to 0.09375
- w_down: bfloat16 [18944, 3584], P('seq', 'mp'), may hold values from -0.125 to 0.125
Outputs:
- attended: bfloat16 [256, 3584], P('mp', 'seq')
- layer_out: bfloat16 [256, 3584], P('mp', 'seq')
The draws below stay inside these ranges and needn't reach their ends.
All inputs are finite; a program needn't handle non-finite values.
Results may differ from the reference program's by a relative error of at most 0.012.
The reference program's roundings to bfloat16 on the way (of `normed`, `queries`, `normed_ffn` and `activated`) count: a program that leaves them out, or rounds other values in their place, can miss the bound.
Values may be sent and summed in bfloat16 or wider, within the bound.
A program may use at most 64 MiB of HBM per device.

```python
import jax
import jax.numpy as jnp
from jax import lax

D = 3584
HEADS = 28
KV_HEADS = 4
HEAD = 128
FF = 18944
CTX_DEV = 1024
QUERIES = 256
CONTEXT = 65536
N_SEQ = 64


def draw_cache_keys(key, part):
    shape = (KV_HEADS, CONTEXT, HEAD)
    base_key, heavy_key, pick_key = jax.random.split(jax.random.fold_in(key, 17), 3)
    drawn = jnp.clip(2.7 * jax.random.normal(base_key, shape, jnp.float32), -16.0, 16.0)
    return drawn.astype(jnp.bfloat16)


def raised(values, own_key, source, target, blocks, factor):
    def block_of(axis_at):
        return (jnp.arange(values.shape[axis_at]) // (values.shape[axis_at] // blocks)).reshape((-1,) + (1,) * (values.ndim - 1 - axis_at))

    first = jax.random.permutation(own_key, blocks)[block_of(target)]
    far = (block_of(target) + blocks // 2) % blocks
    return jnp.where((block_of(source) == first) | (block_of(source) == far), factor * values, values)


def shard_levels(rng, extent, cuts, least, largest):
    loudness = 1.0
    for axis_at, blocks in cuts:
        draws = jax.random.uniform(jax.random.fold_in(jax.random.fold_in(rng, 6), axis_at), (blocks,), jnp.float32, least / len(cuts), largest / len(cuts))
        loudness = loudness * jnp.repeat(jnp.exp(draws), extent[axis_at] // blocks).reshape((-1,) + (1,) * (len(extent) - 1 - axis_at))
    return loudness


def centred(stream_key, extent, width, most, cuts=(), held_as=jnp.bfloat16):
    loudness = shard_levels(stream_key, extent, cuts, -0.22, 0.18) if cuts else 1.0
    values = jax.random.normal(stream_key, extent, jnp.float32) * width * loudness
    return jnp.minimum(jnp.maximum(values, -most), most).astype(held_as)


def heavy_noise(rng, dims, spread, most, cuts, heavy, kind=jnp.bfloat16):
    entries = spread * jax.random.normal(rng, dims, jnp.float32)
    if cuts:
        entries = entries * shard_levels(rng, dims, cuts, -0.22, 0.18)
    return jnp.clip(raised(entries, jax.random.fold_in(rng, 3), *heavy), -most, most).astype(kind)


def setup_inputs(seed: int = 0) -> dict:
    keys = jax.random.split(jax.random.key(seed), 12)
    return {
        "tokens": centred(keys[0], (QUERIES, D), 1.0, 6.0, ((0, 4),)),
        "gain_attn": jnp.clip(1.0 + 0.15 * jax.random.normal(keys[1], (D,), jnp.float32), 0.25, 1.75),
        "w_query": centred(keys[2], (D, D), D ** -0.5, 0.09375, ((1, 64),)),
        "query_bias": centred(keys[3], (D,), 0.5, 3.0, ((0, 64),), jnp.float32),
        "cache_keys": draw_cache_keys(jax.random.fold_in(keys[11], 71), 0),
        "cache_values": centred(keys[5], (KV_HEADS, CONTEXT, HEAD), 1.0, 6.0, ((1, 64),)),
        "w_out": centred(keys[6], (D, D), D ** -0.5, 0.09375, ((1, 64),)),
        "gain_ffn": jnp.clip(1.0 + 0.15 * jax.random.normal(keys[7], (D,), jnp.float32), 0.25, 1.75),
        "w_gate": centred(keys[8], (D, FF), D ** -0.5, 0.09375, ((0, 4), (1, 64))),
        "w_up": centred(keys[9], (D, FF), D ** -0.5, 0.09375, ((0, 4), (1, 64))),
        "w_down": heavy_noise(keys[10], (FF, D), FF ** -0.5, 0.125, ((0, 64), (1, 4)), (0, 1, 64, 4.0)),
    }


eps = 1e-06

def expand(per_head):
    return jnp.repeat(per_head, HEAD, axis=1)

def block_attention(queries, block_keys, block_values):
    row_count = queries.shape[0]
    group_size = HEADS // KV_HEADS
    shaped = queries.reshape(row_count, KV_HEADS, group_size * HEAD)
    maxima = []
    sums = []
    outputs = []
    for head_group in range(KV_HEADS):
        block_query = shaped[:, head_group, :].reshape(row_count * group_size, HEAD)
        scores = jnp.einsum('rd,kd->rk', block_query.astype(jnp.float32), block_keys[head_group].astype(jnp.float32)) * HEAD ** (-0.5)
        highest = lax.optimization_barrier(jnp.max(scores, axis=1, keepdims=True))
        probs = jnp.exp(scores - highest)
        weight_sum = lax.optimization_barrier(jnp.sum(probs, axis=1))
        weighted = jnp.dot(probs.astype(jnp.bfloat16), block_values[head_group], preferred_element_type=jnp.float32)
        maxima.append(highest.reshape(row_count, group_size))
        sums.append(weight_sum.reshape(row_count, group_size))
        outputs.append(weighted.reshape(row_count, group_size * HEAD))
    return (jnp.concatenate(maxima, axis=1), jnp.concatenate(sums, axis=1), jnp.concatenate(outputs, axis=1))

def combine(first, second):
    highest = jnp.maximum(first[0], second[0])
    scale_one = jnp.exp(first[0] - highest)
    scale_two = jnp.exp(second[0] - highest)
    weight_sum = first[1] * scale_one + second[1] * scale_two
    weighted = first[2] * expand(scale_one) + second[2] * expand(scale_two)
    return (highest, weight_sum, weighted)

def reference(tokens, gain_attn, w_query, query_bias, cache_keys, cache_values, w_out, gain_ffn, w_gate, w_up, w_down):
    hidden_in = tokens.astype(jnp.float32)
    mean_sq = lax.optimization_barrier(jnp.mean(hidden_in * hidden_in, axis=1, keepdims=True))
    normed = (hidden_in * lax.rsqrt(mean_sq + eps) * gain_attn).astype(jnp.bfloat16)
    queries = (jnp.dot(normed, w_query, preferred_element_type=jnp.float32) + query_bias).astype(jnp.bfloat16)
    key_blocks = cache_keys.reshape(KV_HEADS, N_SEQ, CTX_DEV, HEAD).transpose(1, 0, 2, 3)
    value_blocks = cache_values.reshape(KV_HEADS, N_SEQ, CTX_DEV, HEAD).transpose(1, 0, 2, 3)
    start_state = block_attention(queries, key_blocks[0], value_blocks[0])

    def absorb(carried, blocks):
        return (combine(carried, block_attention(queries, blocks[0], blocks[1])), None)
    final_state, unused = lax.scan(absorb, start_state, (key_blocks[1:], value_blocks[1:]))
    attended = (final_state[2] / expand(final_state[1])).astype(jnp.bfloat16)
    residual = hidden_in + jnp.dot(attended, w_out, preferred_element_type=jnp.float32)
    mean_res = lax.optimization_barrier(jnp.mean(residual * residual, axis=1, keepdims=True))
    normed_ffn = (residual * lax.rsqrt(mean_res + eps) * gain_ffn).astype(jnp.bfloat16)
    gate_proj = jnp.dot(normed_ffn, w_gate, preferred_element_type=jnp.float32)
    up_proj = jnp.dot(normed_ffn, w_up, preferred_element_type=jnp.float32)
    activated = (jax.nn.silu(gate_proj) * up_proj).astype(jnp.bfloat16)
    ffn_sum = jnp.dot(activated, w_down, preferred_element_type=jnp.float32)
    layer_out = (residual + ffn_sum).astype(jnp.bfloat16)
    return (attended, layer_out)
```

```python
import functools
import math

import jax
import jax.numpy as jnp
from jax import lax
from jax.experimental import pallas as pl
from jax.experimental.pallas import tpu as pltpu
from jax.sharding import PartitionSpec as P

D = 3584
HEAD = 128
GROUP = 7
KV = 4
CTX = 1024
SEQ = 64
MP = 4
TOK = 64
ALL = TOK * MP
COL = 56
FEAT = D // MP
PEER = FEAT // COL
HID = 296
QUART = 80
HIDP = QUART * MP
PK = 32
EPS = 1e-06
MESH = pl.DeviceIdType.MESH
BF = jnp.bfloat16
F32 = jnp.float32
LOG2E = 1.0 / math.log(2.0)


def dot(a, b, dims=((1,), (0,))):
    return lax.dot_general(a, b, (dims, ((), ())), preferred_element_type=F32)


def low_lanes(rows):
    return lax.broadcasted_iota(jnp.int32, (rows, 128), 1) < 64


def row_ids(rows):
    return lax.broadcasted_iota(jnp.int32, (rows, 128), 0)


def swap(x):
    return pltpu.roll(x, 64, axis=1)


def column_of(row):
    n = row.shape[1]
    same = lax.broadcasted_iota(jnp.int32, (n, n), 0) == lax.broadcasted_iota(jnp.int32, (n, n), 1)
    return jnp.sum(jnp.where(same, jnp.broadcast_to(row, (n, n)), 0.0), axis=1, keepdims=True)


def split3(x):
    first = x.astype(BF).astype(F32)
    rest = x - first
    second = rest.astype(BF).astype(F32)
    return first, second, rest - second


def three_rows(x, rows, base=0):
    first, second, third = split3(x)
    at = lax.broadcasted_iota(jnp.int32, (rows, x.shape[1]), 0) - base
    return jnp.where(at == 0, first, jnp.where(at == 1, second, jnp.where(at == 2, third, 0.0)))


def kernel(
    tokens_h, gain_attn_h, wq_h, bias_h, keys_h, values_h, wo_h, gain_ffn_h, wg_h, wu_h, wd_h,
    att_out, lay_out,
    tokens, gain_attn, wq, bias, keys, values, wo, gain_ffn, wg, wu, wd,
    normed, value_t, wd_t, hid_t, work, outs, lsplit, stage1, stage2, stage4, stage6,
    buf1, buf2, buf3, buf4, buf6, la, lb, att3, gu, gstage, gbuf, act, res,
    in_sem, ssem, rsem, asem,
):
    s = lax.axis_index("seq")
    m = lax.axis_index("mp")
    own_m = s // PEER
    own_j = lax.rem(s, PEER)
    mine = own_m == m

    pairs = (
        (tokens_h, tokens), (gain_attn_h, gain_attn), (wq_h, wq), (bias_h, bias),
        (keys_h.at[m], keys), (values_h.at[m], values), (wo_h, wo), (gain_ffn_h, gain_ffn),
        (wg_h, wg), (wu_h, wu), (wd_h, wd.at[pl.ds(0, HID)]),
    )
    loads = [pltpu.make_async_copy(a, b, in_sem.at[i]) for i, (a, b) in enumerate(pairs)]
    for load in loads:
        load.start()

    bar = pltpu.get_barrier_semaphore()

    def greet(p, q):
        pl.semaphore_signal(bar, inc=1, device_id=(p, q), device_id_type=MESH)

    def greet_all(i, c):
        j, q = i // MP, lax.rem(i, MP)

        @pl.when(jnp.logical_not(jnp.logical_and(PEER * m + j == s, q == m)))
        def _():
            greet(PEER * m + j, q)

        @pl.when(jnp.logical_not(jnp.logical_and(i == s, own_m == m)))
        def _():
            greet(i, own_m)

        @pl.when(i != s)
        def _():
            greet(i, m)

        return c

    lax.fori_loop(0, SEQ, greet_all, 0)
    for d in range(1, MP):
        greet(s, lax.rem(m + d, MP))

    loads[0].wait()
    loads[1].wait()
    normed[pl.ds(TOK, TOK), :] = jnp.zeros((TOK, D), BF)

    def norm_rows(i, c):
        at = pl.multiple_of(i * 16, 16)
        x = tokens[pl.ds(at, 16), :].astype(F32)
        mean_sq = jnp.sum(x * x, axis=1, keepdims=True) * (1.0 / D)
        normed[pl.ds(at, 16), :] = (x * lax.rsqrt(mean_sq + EPS) * gain_attn[...]).astype(BF)
        return c

    lax.fori_loop(0, TOK // 16, norm_rows, 0)
    loads[2].wait()
    loads[3].wait()
    q_t = dot(wq[...], normed[...], ((1,), (1,))) + column_of(bias[...])
    low32 = low_lanes(PK)

    def packed(x):
        hi = jnp.concatenate([x[PK:COL], jnp.zeros((8, 128), F32)], axis=0)
        return jnp.where(low32, x[0:PK], swap(hi))

    stage1[...] = packed(q_t).astype(BF)
    pl.semaphore_wait(bar, jnp.where(mine, 2 * SEQ - 2, 2 * SEQ) + SEQ - 1 + MP - 1)

    slot1 = own_j * MP + m

    def gather_to_users(stage, buf, k):
        def send(i, c):
            p = lax.rem(s + i, SEQ)
            local = jnp.logical_and(p == s, mine)

            @pl.when(local)
            def _():
                pltpu.make_async_copy(stage, buf.at[slot1], rsem.at[k]).start()

            @pl.when(jnp.logical_not(local))
            def _():
                pltpu.make_async_remote_copy(
                    src_ref=stage, dst_ref=buf.at[slot1], send_sem=ssem.at[k], recv_sem=rsem.at[k],
                    device_id=(p, own_m), device_id_type=MESH,
                ).start()

            return c

        lax.fori_loop(1, SEQ + 1, send, 0)

    def scatter_to_owners(stage, buf, k):
        def send(i, c):
            at = lax.rem(own_j * MP + m + i, SEQ)
            j, q = at // MP, lax.rem(at, MP)
            p = PEER * m + j
            local = jnp.logical_and(p == s, q == m)

            @pl.when(local)
            def _():
                pltpu.make_async_copy(stage.at[at], buf.at[s], rsem.at[k]).start()

            @pl.when(jnp.logical_not(local))
            def _():
                pltpu.make_async_remote_copy(
                    src_ref=stage.at[at], dst_ref=buf.at[s], send_sem=ssem.at[k], recv_sem=rsem.at[k],
                    device_id=(p, q), device_id_type=MESH,
                ).start()

            return c

        lax.fori_loop(1, SEQ + 1, send, 0)

    def arrived(buf, k):
        pltpu.make_async_copy(buf, buf, rsem.at[k]).wait()

    def sent(buf, k):
        @pl.when(mine)
        def _():
            some = buf.at[pl.ds(0, SEQ - 1)]
            pltpu.make_async_copy(some, some, ssem.at[k]).wait()

        @pl.when(jnp.logical_not(mine))
        def _():
            pltpu.make_async_copy(buf, buf, ssem.at[k]).wait()

    gather_to_users(stage1, buf1, 0)

    first = lax.broadcasted_iota(jnp.int32, (COL, D), 1) - lax.broadcasted_iota(jnp.int32, (COL, D), 0)
    pick = jnp.where(first == s * COL, 1.0, 0.0).astype(BF)
    loads[5].wait()
    value_t[...] = values[...].T
    normed[pl.ds(0, TOK), :] = tokens[...]
    hid_t[...] = dot(pick, normed[...], ((1,), (1,)))
    loads[10].wait()
    wd[pl.ds(HID, HIDP - HID), :] = jnp.zeros((HIDP - HID, FEAT), BF)
    wd_t[...] = wd[...].T
    outs[pl.ds(FEAT, 8), :] = jnp.zeros((8, ALL), F32)
    gu[:, pl.ds(HID, HIDP - HID), :] = jnp.zeros((2, HIDP - HID, ALL), F32)
    for i in (4, 6, 7, 8, 9):
        loads[i].wait()

    def unpack_chunks(buf, squares):
        def one(j, sums):
            sums = list(sums)
            for t in range(2):
                a = buf[j * MP + 2 * t].astype(F32)
                b = buf[j * MP + 2 * t + 1].astype(F32)
                lo = jnp.where(low32, a, swap(b))
                hi = jnp.where(low32, swap(a), b)
                at = pl.multiple_of(j * COL, 8)
                work[pl.ds(at, PK), pl.ds(128 * t, 128)] = lo
                work[pl.ds(pl.multiple_of(at + PK, 8), COL - PK), pl.ds(128 * t, 128)] = hi[0 : COL - PK]
                if squares:
                    sums[t] = sums[t] + hi[COL - PK : PK]
            return tuple(sums)

        zero = jnp.zeros((8, 128), F32)
        return lax.fori_loop(0, PEER, one, (zero, zero))

    def pack_chunks(stage, stats):
        def one(j, c):
            at = pl.multiple_of(j * COL, 8)
            for t in range(2):
                r = outs[pl.ds(at, 2 * PK), pl.ds(128 * t, 128)]
                lo, hi = r[0:PK], r[PK : 2 * PK]
                a = jnp.where(low32, lo, swap(hi))
                b = jnp.where(low32, swap(lo), hi)
                if stats:
                    h0, h1 = (j * COL) // HEAD, (j * COL + COL - 1) // HEAD
                    low8 = low_lanes(8)
                    both = jnp.where(
                        row_ids(8) < 3, lsplit[h0, :, pl.ds(128 * t, 128)], lsplit[h1, :, pl.ds(128 * t, 128)]
                    )
                    a = jnp.concatenate([a[0:24], jnp.where(low8, a[24:PK], swap(both))], axis=0)
                    b = jnp.concatenate([b[0:24], jnp.where(low8, b[24:PK], both)], axis=0)
                stage[j * MP + 2 * t] = a.astype(BF)
                stage[j * MP + 2 * t + 1] = b.astype(BF)
            return c

        lax.fori_loop(0, PEER, one, 0)

    arrived(buf1, 0)
    unpack_chunks(buf1, False)
    scale = HEAD ** (-0.5) * LOG2E

    def one_head(h, c):
        at = pl.multiple_of(h * HEAD, HEAD)
        scores = dot(keys[...], work[pl.ds(at, HEAD), :].astype(BF)) * scale
        top = jnp.max(scores, axis=0, keepdims=True)
        probs = jnp.exp2(scores - top)
        total = jnp.sum(probs, axis=0, keepdims=True)
        outs[pl.ds(at, HEAD), :] = dot(value_t[...], probs.astype(BF)) * (1.0 / total)
        level = top + jnp.log(total) * LOG2E
        lsplit[h] = three_rows(level, 8) + three_rows(level, 8, 3)
        return c

    lax.fori_loop(0, GROUP, one_head, 0)
    pack_chunks(stage2, True)
    scatter_to_owners(stage2, buf2, 1)

    arrived(buf2, 1)
    low128 = low_lanes(SEQ)

    def levels(i, c):
        part = buf2[i, pl.ds(16, 16), :].astype(F32)[8:16]
        at = row_ids(8)
        la[pl.ds(i, 1), :] = jnp.sum(jnp.where(at < 3, part, 0.0), axis=0, keepdims=True)
        lb[pl.ds(i, 1), :] = jnp.sum(
            jnp.where(jnp.logical_and(at >= 3, at < 6), part, 0.0), axis=0, keepdims=True
        )
        return c

    lax.fori_loop(0, SEQ, levels, 0)
    for ref in (la, lb):
        level = ref[...]
        level = jnp.where(low128, swap(level), level)
        weight = jnp.exp2(level - jnp.max(level, axis=0, keepdims=True))
        ref[...] = weight / jnp.sum(weight, axis=0, keepdims=True)
    edge = HEAD * ((own_j * COL) // HEAD + 1) - own_j * COL
    first_head = row_ids(PK) + jnp.where(low32, 0, PK) < edge

    def combine(i, acc):
        return acc + buf2[i].astype(F32) * jnp.where(first_head, la[pl.ds(i, 1), :], lb[pl.ds(i, 1), :])

    merged = lax.fori_loop(0, SEQ, combine, jnp.zeros((PK, 128), F32)).astype(BF)
    buf3[s] = merged

    def send3(i, c):
        pltpu.make_async_remote_copy(
            src_ref=buf3.at[s], dst_ref=buf3.at[s], send_sem=ssem.at[2], recv_sem=rsem.at[2],
            device_id=(lax.rem(s + i, SEQ), m), device_id_type=MESH,
        ).start()
        return c

    lax.fori_loop(1, SEQ, send3, 0)

    def unpacked(x, out):
        out[pl.ds(0, PK), :] = x[:, 0:64].astype(BF)
        out[pl.ds(PK, COL - PK), :] = swap(x)[0 : COL - PK, 0:64].astype(BF)

    unpacked(merged.astype(F32), att_out)
    res_hid = packed(hid_t[...])
    gain_pk = packed(jnp.broadcast_to(column_of(gain_ffn[...]), (COL, 128)))
    gain_pk = jnp.where(low32, gain_pk, packed(swap(jnp.broadcast_to(column_of(gain_ffn[...]), (COL, 128)))))
    others = buf3.at[pl.ds(0, SEQ - 1)]
    pltpu.make_async_copy(others, others, rsem.at[2]).wait()

    def spread(i, c):
        x = buf3[i].astype(F32)
        at = pl.multiple_of(i * COL, 8)
        att3[pl.ds(at, PK), :] = x
        att3[pl.ds(pl.multiple_of(at + PK, 8), COL - PK), :] = swap(x)[0 : COL - PK]
        return c

    lax.fori_loop(0, SEQ, spread, 0)
    projected = jnp.zeros((COL, 128), F32)
    for i in range(4):
        projected += dot(wo[:, pl.ds(i * FEAT, FEAT)], att3[pl.ds(i * FEAT, FEAT), :].astype(BF))
    residual = res_hid + packed(projected)
    res[...] = residual

    real = jnp.logical_or(low32, row_ids(PK) < COL - PK)
    squares = jnp.sum(jnp.where(real, residual * residual, 0.0), axis=0, keepdims=True)
    squares = squares + swap(squares)
    scaled = residual * gain_pk
    stage4[...] = jnp.where(real, scaled, three_rows(squares, PK, 24)).astype(BF)
    gather_to_users(stage4, buf4, 3)
    arrived(buf4, 3)
    sums = unpack_chunks(buf4, True)
    sq = jnp.concatenate([jnp.sum(x, axis=0, keepdims=True) for x in sums], axis=1)

    features = work[pl.ds(0, FEAT), :].astype(BF)
    gu[0, pl.ds(0, HID), :] = dot(wg[...], features)
    gu[1, pl.ds(0, HID), :] = dot(wu[...], features)
    sq_rows = three_rows(sq, 16).astype(BF)
    for d in range(1, MP):
        q = lax.rem(m + d, MP)
        at = pl.multiple_of(q * QUART, 16)
        gstage[d, pl.ds(0, QUART), :] = gu[0, pl.ds(at, QUART), :].astype(BF)
        gstage[d, pl.ds(QUART, QUART), :] = gu[1, pl.ds(at, QUART), :].astype(BF)
        gstage[d, pl.ds(2 * QUART, 16), :] = sq_rows
        pltpu.make_async_remote_copy(
            src_ref=gstage.at[d], dst_ref=gbuf.at[d], send_sem=asem.at[0, d], recv_sem=asem.at[1, d],
            device_id=(s, q), device_id_type=MESH,
        ).start()
    at = pl.multiple_of(m * QUART, 16)
    gate = gu[0, pl.ds(at, QUART), :]
    up = gu[1, pl.ds(at, QUART), :]
    for d in range(1, MP):
        pltpu.make_async_copy(gbuf.at[d], gbuf.at[d], asem.at[1, d]).wait()
        gate += gbuf[d, pl.ds(0, QUART), :].astype(F32)
        up += gbuf[d, pl.ds(QUART, QUART), :].astype(F32)
        sq += jnp.sum(gbuf[d, pl.ds(2 * QUART, 16), :].astype(F32), axis=0, keepdims=True)
    factor = lax.rsqrt(sq * (1.0 / D) + EPS)
    gate = gate * factor
    up = up * factor
    act[pl.ds(at, QUART), :] = (gate / (1.0 + jnp.exp(-gate)) * up).astype(BF)
    for d in range(1, MP):
        q = lax.rem(m + d, MP)
        pltpu.make_async_remote_copy(
            src_ref=act.at[pl.ds(at, QUART)], dst_ref=act.at[pl.ds(at, QUART)],
            send_sem=asem.at[2, d], recv_sem=asem.at[3, d], device_id=(s, q), device_id_type=MESH,
        ).start()
    for d in range(1, MP):
        src = act.at[pl.ds(pl.multiple_of(lax.rem(m + MP - d, MP) * QUART, 16), QUART)]
        pltpu.make_async_copy(src, src, asem.at[3, d]).wait()

    outs[pl.ds(0, FEAT), :] = dot(wd_t[...], act[...])
    pack_chunks(stage6, False)
    scatter_to_owners(stage6, buf6, 4)
    arrived(buf6, 4)

    def add(i, acc):
        return acc + buf6[i].astype(F32)

    unpacked(lax.fori_loop(0, SEQ, add, res[...]), lay_out)

    for k, buf in ((0, buf1), (1, buf2), (3, buf4), (4, buf6)):
        sent(buf, k)
    pltpu.make_async_copy(others, others, ssem.at[2]).wait()
    for d in range(1, MP):
        pltpu.make_async_copy(gstage.at[d], gstage.at[d], asem.at[0, d]).wait()
        src = act.at[pl.ds(at, QUART)]
        pltpu.make_async_copy(src, src, asem.at[2, d]).wait()


def body(tokens, gain_attn, w_query, query_bias, cache_keys, cache_values, w_out, gain_ffn, w_gate, w_up, w_down):
    v = pltpu.VMEM
    chunk = (SEQ, PK, 128)
    scratch = [
        v((TOK, D), BF), v((1, D), F32), v((COL, D), BF), v((1, COL), F32), v((CTX, HEAD), BF), v((CTX, HEAD), BF),
        v((COL, D), BF), v((1, COL), F32), v((HID, FEAT), BF), v((HID, FEAT), BF), v((HIDP, FEAT), BF),
        v((2 * TOK, D), BF),
        v((HEAD, CTX), BF),
        v((FEAT, HIDP), BF),
        v((COL, 128), F32),
        v((FEAT, ALL), F32),
        v((FEAT + 8, ALL), F32),
        v((8, 8, ALL), F32),
        v((PK, 128), BF), v(chunk, BF), v((PK, 128), BF), v(chunk, BF),
        v(chunk, BF), v(chunk, BF), v(chunk, BF), v(chunk, BF), v(chunk, BF),
        v((SEQ, 128), F32), v((SEQ, 128), F32),
        v((D, 128), F32),
        v((2, HIDP, ALL), F32),
        v((MP, 2 * QUART + 16, ALL), BF), v((MP, 2 * QUART + 16, ALL), BF),
        v((HIDP, ALL), BF),
        v((PK, 128), F32),
        pltpu.SemaphoreType.DMA((11,)),
        pltpu.SemaphoreType.DMA((5,)),
        pltpu.SemaphoreType.DMA((5,)),
        pltpu.SemaphoreType.DMA((4, MP)),
    ]
    any_space = pl.BlockSpec(memory_space=pl.ANY)
    attended, layer = pl.pallas_call(
        kernel,
        out_shape=(jax.ShapeDtypeStruct((COL, TOK), BF), jax.ShapeDtypeStruct((COL, TOK), BF)),
        in_specs=[any_space] * 11,
        out_specs=(pl.BlockSpec(memory_space=pltpu.VMEM), pl.BlockSpec(memory_space=pltpu.VMEM)),
        scratch_shapes=scratch,
        compiler_params=pltpu.CompilerParams(
            collective_id=0, has_side_effects=True, vmem_limit_bytes=48 * 1024 * 1024
        ),
        name="layer",
    )(
        tokens, gain_attn.reshape(1, D), w_query.T, query_bias.reshape(1, COL), cache_keys, cache_values,
        w_out.T, gain_ffn.reshape(1, COL), w_gate.T, w_up.T, w_down,
    )
    return attended.T, layer.T


def solution(mesh):
    placed = (
        P("mp", None), P(), P(None, "seq"), P("seq"), P(None, "seq", None), P(None, "seq", None),
        P(None, "seq"), P("seq"), P("mp", "seq"), P("mp", "seq"), P("seq", "mp"),
    )
    return jax.shard_map(
        body, mesh=mesh, in_specs=placed, out_specs=(P("mp", "seq"), P("mp", "seq")), check_vma=False
    )
```

```python
import functools
import math

import jax
import jax.numpy as jnp
from jax import lax
from jax.experimental import pallas as pl
from jax.experimental.pallas import tpu as pltpu
from jax.sharding import PartitionSpec as P

D = 3584
HEAD = 128
GROUP = 7
KV = 4
CTX = 1024
SEQ = 64
MP = 4
TOK = 64
ALL = TOK * MP
COL = 56
FEAT = D // MP
PEER = FEAT // COL
HID = 296
QUART = 80
HIDP = QUART * MP
PK = 32
LINE = 8
EPS = 1e-06
MESH = pl.DeviceIdType.MESH
BF = jnp.bfloat16
F32 = jnp.float32
LOG2E = 1.0 / math.log(2.0)


def dot(a, b, dims=((1,), (0,))):
    return lax.dot_general(a, b, (dims, ((), ())), preferred_element_type=F32)


def low_lanes(rows):
    return lax.broadcasted_iota(jnp.int32, (rows, 128), 1) < 64


def row_ids(rows):
    return lax.broadcasted_iota(jnp.int32, (rows, 128), 0)


def swap(x):
    return pltpu.roll(x, 64, axis=1)


def column_of(row):
    n = row.shape[1]
    same = lax.broadcasted_iota(jnp.int32, (n, n), 0) == lax.broadcasted_iota(jnp.int32, (n, n), 1)
    return jnp.sum(jnp.where(same, jnp.broadcast_to(row, (n, n)), 0.0), axis=1, keepdims=True)


def split3(x):
    first = x.astype(BF).astype(F32)
    rest = x - first
    second = rest.astype(BF).astype(F32)
    return first, second, rest - second


def three_rows(x, rows, base=0):
    first, second, third = split3(x)
    at = lax.broadcasted_iota(jnp.int32, (rows, x.shape[1]), 0) - base
    return jnp.where(at == 0, first, jnp.where(at == 1, second, jnp.where(at == 2, third, 0.0)))


def merge_eight(chunks, j):
    at = row_ids(8)
    high = jnp.logical_not(low_lanes(8))
    sides = ([], [])
    for i in range(8):
        part = chunks[i, 24:PK]
        sides[0].append(jnp.sum(jnp.where(at < 3, part, 0.0), axis=0, keepdims=True))
        sides[1].append(jnp.sum(jnp.where(jnp.logical_and(at >= 3, at < 6), part, 0.0), axis=0, keepdims=True))
    weights, levels = [], []
    for rows in sides:
        level = jnp.concatenate(rows, axis=0)
        level = jnp.where(high, level, swap(level))
        top = jnp.max(level, axis=0, keepdims=True)
        weight = jnp.exp2(level - top)
        total = jnp.sum(weight, axis=0, keepdims=True)
        weights.append(weight / total)
        levels.append(top + jnp.log(total) * LOG2E)
    edge = HEAD * ((j * COL) // HEAD + 1) - j * COL
    first_head = row_ids(PK) + jnp.where(low_lanes(PK), 0, PK) < edge
    acc = jnp.zeros((PK, 128), F32)
    for i in range(8):
        acc += chunks[i] * jnp.where(first_head, weights[0][i : i + 1], weights[1][i : i + 1])
    return acc, levels


def kernel(
    tokens_h, gain_attn_h, wq_h, bias_h, keys_h, values_h, wo_h, gain_ffn_h, wg_h, wu_h, wd_h,
    att_out, lay_out,
    tokens, gain_attn, wq, bias, keys, values, wo, gain_ffn, wg, wu, wd,
    normed, value_t, wd_t, hid_t, wo_e, work, outs, lsplit, stage2, stage6,
    line1, line3, line4, buf1, buf3, buf4, plane2, plane6, rel2, rel6, line2, line6,
    gu, gstage, gbuf, act, res,
    in_sem, zsend, zrecv, psend, precv, rrecv, asem,
):
    s = lax.axis_index("seq")
    m = lax.axis_index("mp")
    own_m = s // PEER
    own_j = lax.rem(s, PEER)
    z = lax.rem(s, LINE)
    line = s - z
    here = s // LINE
    mine = own_m == m
    group = (own_j // LINE) * MP + m

    pairs = (
        (tokens_h, tokens), (gain_attn_h, gain_attn), (wq_h, wq), (bias_h, bias),
        (keys_h.at[m], keys), (values_h.at[m], values), (wo_h, wo), (gain_ffn_h, gain_ffn),
        (wg_h, wg), (wu_h, wu), (wd_h, wd.at[pl.ds(0, HID)]),
    )
    loads = [pltpu.make_async_copy(a, b, in_sem.at[i]) for i, (a, b) in enumerate(pairs)]
    for load in loads:
        load.start()

    bar = pltpu.get_barrier_semaphore()

    def greet(p, q):
        pl.semaphore_signal(bar, inc=1, device_id=(p, q), device_id_type=MESH)

    for d in range(1, LINE):
        greet(line + lax.rem(z + d, LINE), m)
    for g in range(8):
        p, q = PEER * m + LINE * (g // MP) + z, g % MP
        local = jnp.logical_and(p == s, q == m)

        @pl.when(jnp.logical_not(local))
        def _(p=p, q=q):
            greet(p, q)

        @pl.when(jnp.logical_not(jnp.logical_and(here == g, mine)))
        def _(g=g):
            greet(LINE * g + z, own_m)

    for d in range(1, 8):
        greet(LINE * lax.rem(here + d, 8) + z, m)
    for d in range(1, MP):
        greet(s, lax.rem(m + d, MP))

    loads[0].wait()
    loads[1].wait()
    normed[pl.ds(TOK, TOK), :] = jnp.zeros((TOK, D), BF)
    gain_row = jnp.concatenate([gain_attn[i : i + 1, :] for i in range(D // 128)], axis=1)

    def norm_rows(i, c):
        at = pl.multiple_of(i * 16, 16)
        x = tokens[pl.ds(at, 16), :].astype(F32)
        mean_sq = jnp.sum(x * x, axis=1, keepdims=True) * (1.0 / D)
        normed[pl.ds(at, 16), :] = (x * lax.rsqrt(mean_sq + EPS) * gain_row).astype(BF)
        return c

    lax.fori_loop(0, TOK // 16, norm_rows, 0)
    loads[2].wait()
    loads[3].wait()
    q_t = dot(wq[...], normed[...], ((1,), (1,))) + column_of(bias[...])
    low32 = low_lanes(PK)

    def packed(x):
        hi = jnp.concatenate([x[PK:COL], jnp.zeros((8, 128), F32)], axis=0)
        return jnp.where(low32, x[0:PK], swap(hi))

    def along_line(held, k):
        for d in (4, 3, 5, 2, 6, 1, 7):
            pltpu.make_async_remote_copy(
                src_ref=held.at[z], dst_ref=held.at[z], send_sem=zsend.at[k], recv_sem=zrecv.at[k, LINE - d],
                device_id=(line + lax.rem(z + d, LINE), m), device_id_type=MESH,
            ).start()

    def on_to_plane(held, buf, k, target, place, own, first, last):
        def step(i, c):
            e = lax.rem(jnp.where(lax.rem(i, 2) == 1, (i + 1) // 2, LINE - i // 2), LINE)
            at = lax.rem(z + e, LINE)

            @pl.when(i > 0)
            def _():
                pltpu.make_async_copy(held.at[at], held.at[at], zrecv.at[k, e]).wait()

            for d in range(1, 8):
                p = lax.rem(here + d, 8)
                pltpu.make_async_remote_copy(
                    src_ref=held.at[at], dst_ref=buf.at[place, at], send_sem=psend.at[k], recv_sem=precv.at[k],
                    device_id=(LINE * p + z, target), device_id_type=MESH,
                ).start()

            @pl.when(own)
            def _():
                pltpu.make_async_copy(held.at[at], buf.at[place, at], precv.at[k]).start()

            @pl.when(jnp.logical_not(own))
            def _():
                pltpu.make_async_remote_copy(
                    src_ref=held.at[at], dst_ref=buf.at[place, at], send_sem=psend.at[k], recv_sem=precv.at[k],
                    device_id=(s, target), device_id_type=MESH,
                ).start()

            return c

        lax.fori_loop(first, last, step, 0)

    def arrived(buf, sem):
        pltpu.make_async_copy(buf, buf, sem).wait()

    def sent(buf, sem, own):
        @pl.when(own)
        def _():
            arrived(buf.at[pl.ds(0, 7)], sem)

        @pl.when(jnp.logical_not(own))
        def _():
            arrived(buf, sem)

    line1[z] = packed(q_t).astype(BF)
    pl.semaphore_wait(bar, 7 + jnp.where(mine, 14, 16) + 7 + MP - 1)
    along_line(line1, 0)
    on_to_plane(line1, buf1, 0, own_m, group, mine, 0, 1)

    loads[5].wait()
    value_t[...] = values[...].T
    on_to_plane(line1, buf1, 0, own_m, group, mine, 1, LINE)
    first = lax.broadcasted_iota(jnp.int32, (COL, D), 1) - lax.broadcasted_iota(jnp.int32, (COL, D), 0)
    pick = jnp.where(first == s * COL, 1.0, 0.0).astype(BF)
    normed[pl.ds(0, TOK), :] = tokens[...]
    hid_t[...] = dot(pick, normed[...], ((1,), (1,)))
    loads[10].wait()
    wd[pl.ds(HID, HIDP - HID), :] = jnp.zeros((HIDP - HID, FEAT), BF)
    wd_t[...] = wd[...].T
    outs[pl.ds(FEAT, 8), :] = jnp.zeros((8, ALL), F32)
    gu[:, pl.ds(HID, HIDP - HID), :] = jnp.zeros((2, HIDP - HID, ALL), F32)
    wide = PEER * PK
    c_at = lax.broadcasted_iota(jnp.int32, (FEAT, wide), 1)
    r_at = lax.broadcasted_iota(jnp.int32, (FEAT, wide), 0) - COL * (c_at // PK)
    c_at = lax.rem(c_at, PK)
    pick_lo = jnp.where(r_at == c_at, 1.0, 0.0).astype(BF)
    pick_hi = jnp.where(jnp.logical_and(r_at == c_at + PK, c_at < COL - PK), 1.0, 0.0).astype(BF)
    wo_e[...] = jnp.zeros((128, SEQ * PK), BF)
    loads[6].wait()
    for i in range(MP):
        part = wo[:, pl.ds(i * FEAT, FEAT)]
        wo_e[pl.ds(0, COL), pl.ds(i * wide, wide)] = dot(part, pick_lo).astype(BF)
        wo_e[pl.ds(64, COL), pl.ds(i * wide, wide)] = dot(part, pick_hi).astype(BF)
    for i in (4, 7, 8, 9):
        loads[i].wait()

    def unpack_chunks(buf, squares):
        def one(j, sums):
            sums = list(sums)
            for t in range(2):
                a = buf[(j // LINE) * MP + 2 * t, lax.rem(j, LINE)].astype(F32)
                b = buf[(j // LINE) * MP + 2 * t + 1, lax.rem(j, LINE)].astype(F32)
                lo = jnp.where(low32, a, swap(b))
                hi = jnp.where(low32, swap(a), b)
                at = pl.multiple_of(j * COL, 8)
                work[pl.ds(at, PK), pl.ds(128 * t, 128)] = lo
                work[pl.ds(pl.multiple_of(at + PK, 8), COL - PK), pl.ds(128 * t, 128)] = hi[0 : COL - PK]
                if squares:
                    sums[t] = sums[t] + hi[COL - PK : PK]
            return tuple(sums)

        zero = jnp.zeros((8, 128), F32)
        return lax.fori_loop(0, PEER, one, (zero, zero), unroll=4)

    low8 = low_lanes(8)

    def far_first(i):
        return lax.rem(LINE + LINE // 2 + jnp.where(lax.rem(i, 2) == 1, -((i + 1) // 2), i // 2), LINE)

    def to_plane(stage, plane, k, stats):
        def step(i, c):
            e = far_first(i)
            to_z = lax.rem(z + e, LINE)
            for half in range(2):
                j = half * LINE + to_z
                at = pl.multiple_of(j * COL, 8)
                for t in range(2):
                    r = outs[pl.ds(at, 2 * PK), pl.ds(128 * t, 128)]
                    lo, hi = r[0:PK], r[PK : 2 * PK]
                    a = jnp.where(low32, lo, swap(hi))
                    b = jnp.where(low32, swap(lo), hi)
                    if stats:
                        h0, h1 = (j * COL) // HEAD, (j * COL + COL - 1) // HEAD
                        both = jnp.where(
                            row_ids(8) < 3, lsplit[h0, :, pl.ds(128 * t, 128)], lsplit[h1, :, pl.ds(128 * t, 128)]
                        )
                        a = jnp.concatenate([a[0:24], jnp.where(low8, a[24:PK], swap(both))], axis=0)
                        b = jnp.concatenate([b[0:24], jnp.where(low8, b[24:PK], both)], axis=0)
                    stage[to_z, half * MP + 2 * t] = a.astype(BF)
                    stage[to_z, half * MP + 2 * t + 1] = b.astype(BF)
            for g in range(8):
                p, q = PEER * m + LINE * (g // MP) + z, g % MP
                local = jnp.logical_and(p == s, q == m)

                @pl.when(local)
                def _():
                    pltpu.make_async_copy(stage.at[to_z, g], plane.at[to_z, here], rrecv.at[k, e]).start()

                @pl.when(jnp.logical_not(local))
                def _():
                    pltpu.make_async_remote_copy(
                        src_ref=stage.at[to_z, g], dst_ref=plane.at[to_z, here],
                        send_sem=psend.at[k], recv_sem=rrecv.at[k, e], device_id=(p, q), device_id_type=MESH,
                    ).start()

            return c

        lax.fori_loop(0, LINE, step, 0)

    def pass_on(plane, rel, held, k, join):
        def step(i, c):
            e = far_first(i)
            to_z = lax.rem(z + e, LINE)
            arrived(plane.at[to_z], rrecv.at[k, e])
            rel[to_z] = join(plane[to_z].astype(F32), to_z).astype(BF)
            pltpu.make_async_remote_copy(
                src_ref=rel.at[to_z], dst_ref=held.at[z], send_sem=zsend.at[k], recv_sem=zrecv.at[k, 0],
                device_id=(line + to_z, m), device_id_type=MESH,
            ).start()
            return c

        lax.fori_loop(0, LINE - 1, step, 0)
        arrived(plane.at[z], rrecv.at[k, 0])
        held[z] = join(plane[z].astype(F32), z).astype(BF)
        arrived(held.at[pl.ds(0, 7)], zrecv.at[k, 0])

    arrived(buf1, precv.at[0])
    unpack_chunks(buf1, False)
    scale = HEAD ** (-0.5) * LOG2E

    def one_head(h, c):
        at = pl.multiple_of(h * HEAD, HEAD)
        scores = dot(keys[...], work[pl.ds(at, HEAD), :].astype(BF)) * scale
        top = jnp.max(scores, axis=0, keepdims=True)
        probs = jnp.exp2(scores - top)
        total = jnp.sum(probs, axis=0, keepdims=True)
        outs[pl.ds(at, HEAD), :] = dot(value_t[...], probs.astype(BF)) * (1.0 / total)
        level = top + jnp.log(total) * LOG2E
        lsplit[h] = three_rows(level, 8) + three_rows(level, 8, 3)
        return c

    lax.fori_loop(0, GROUP, one_head, 0)

    to_plane(stage2, plane2, 1, True)

    def join2(chunks, to_z):
        value, levels = merge_eight(chunks, (own_j // LINE) * LINE + to_z)
        rows = three_rows(levels[0], 8) + three_rows(levels[1], 8, 3)
        return jnp.concatenate([value[0:24], jnp.where(low8, value[24:PK], rows)], axis=0)

    pass_on(plane2, rel2, line2, 1, join2)
    merged = merge_eight(line2[...].astype(F32), own_j)[0].astype(BF)
    line3[z] = merged

    along_line(line3, 2)
    on_to_plane(line3, buf3, 2, m, here, True, 0, LINE)

    def unpacked(x, out):
        out[pl.ds(0, PK), :] = x[:, 0:64].astype(BF)
        out[pl.ds(PK, COL - PK), :] = swap(x)[0 : COL - PK, 0:64].astype(BF)

    unpacked(merged.astype(F32), att_out)
    res_hid = packed(hid_t[...])
    gain_col = jnp.broadcast_to(column_of(gain_ffn[...]), (COL, 128))
    gain_pk = packed(gain_col)
    arrived(buf3, precv.at[2])
    both = dot(wo_e[...], buf3[...].reshape(SEQ * PK, 128))
    residual = res_hid + packed(both[0:COL] + swap(both[64 : 64 + COL]))
    res[...] = residual

    real = jnp.logical_or(low32, row_ids(PK) < COL - PK)
    squares = jnp.sum(jnp.where(real, residual * residual, 0.0), axis=0, keepdims=True)
    squares = squares + swap(squares)
    scaled = residual * gain_pk
    line4[z] = jnp.where(real, scaled, three_rows(squares, PK, 24)).astype(BF)
    along_line(line4, 3)
    on_to_plane(line4, buf4, 3, own_m, group, mine, 0, LINE)
    arrived(buf4, precv.at[3])
    sums = unpack_chunks(buf4, True)
    sq = jnp.concatenate([jnp.sum(x, axis=0, keepdims=True) for x in sums], axis=1)

    features = work[pl.ds(0, FEAT), :].astype(BF)
    gu[0, pl.ds(0, HID), :] = dot(wg[...], features)
    gu[1, pl.ds(0, HID), :] = dot(wu[...], features)
    sq_rows = three_rows(sq, 16).astype(BF)
    for d in range(1, MP):
        q = lax.rem(m + d, MP)
        at = pl.multiple_of(q * QUART, 16)
        gstage[d, pl.ds(0, QUART), :] = gu[0, pl.ds(at, QUART), :].astype(BF)
        gstage[d, pl.ds(QUART, QUART), :] = gu[1, pl.ds(at, QUART), :].astype(BF)
        gstage[d, pl.ds(2 * QUART, 16), :] = sq_rows
        pltpu.make_async_remote_copy(
            src_ref=gstage.at[d], dst_ref=gbuf.at[d], send_sem=asem.at[0, d], recv_sem=asem.at[1, d],
            device_id=(s, q), device_id_type=MESH,
        ).start()
    at = pl.multiple_of(m * QUART, 16)
    gate = gu[0, pl.ds(at, QUART), :]
    up = gu[1, pl.ds(at, QUART), :]
    for d in range(1, MP):
        arrived(gbuf.at[d], asem.at[1, d])
        gate += gbuf[d, pl.ds(0, QUART), :].astype(F32)
        up += gbuf[d, pl.ds(QUART, QUART), :].astype(F32)
        sq += jnp.sum(gbuf[d, pl.ds(2 * QUART, 16), :].astype(F32), axis=0, keepdims=True)
    factor = lax.rsqrt(sq * (1.0 / D) + EPS)
    gate = gate * factor
    up = up * factor
    act[pl.ds(at, QUART), :] = (gate / (1.0 + jnp.exp(-gate)) * up).astype(BF)
    for d in range(1, MP):
        q = lax.rem(m + d, MP)
        pltpu.make_async_remote_copy(
            src_ref=act.at[pl.ds(at, QUART)], dst_ref=act.at[pl.ds(at, QUART)],
            send_sem=asem.at[2, d], recv_sem=asem.at[3, d], device_id=(s, q), device_id_type=MESH,
        ).start()
    for d in range(1, MP):
        arrived(act.at[pl.ds(pl.multiple_of(lax.rem(m + MP - d, MP) * QUART, 16), QUART)], asem.at[3, d])

    outs[pl.ds(0, FEAT), :] = dot(wd_t[...], act[...])
    to_plane(stage6, plane6, 4, False)
    pass_on(plane6, rel6, line6, 4, lambda chunks, to_z: jnp.sum(chunks, axis=0))
    unpacked(res[...] + jnp.sum(line6[...].astype(F32), axis=0), lay_out)

    for k in range(5):
        arrived(line1.at[pl.ds(0, 7)], zsend.at[k])
    for k, buf in ((0, buf1), (1, plane2), (3, buf4), (4, plane6)):
        sent(buf, psend.at[k], mine)
    arrived(buf3.at[pl.ds(0, 7)], psend.at[2])
    for d in range(1, MP):
        arrived(gstage.at[d], asem.at[0, d])
        arrived(act.at[pl.ds(at, QUART)], asem.at[2, d])


def body(tokens, gain_attn, w_query, query_bias, cache_keys, cache_values, w_out, gain_ffn, w_gate, w_up, w_down):
    v = pltpu.VMEM
    eight = (LINE, PK, 128)
    chunks = (8, LINE, PK, 128)
    sem = pltpu.SemaphoreType.DMA
    scratch = [
        v((TOK, D), BF), v((D // 128, 128), F32), v((COL, D), BF), v((1, COL), F32), v((CTX, HEAD), BF),
        v((CTX, HEAD), BF), v((COL, D), BF), v((1, COL), F32), v((HID, FEAT), BF), v((HID, FEAT), BF),
        v((HIDP, FEAT), BF),
        v((2 * TOK, D), BF),
        v((HEAD, CTX), BF),
        v((FEAT, HIDP), BF),
        v((COL, 128), F32),
        v((128, SEQ * PK), BF),
        v((FEAT, ALL), F32),
        v((FEAT + 8, ALL), F32),
        v((8, 8, ALL), F32),
        v(chunks, BF), v(chunks, BF),
        v(eight, BF), v(eight, BF), v(eight, BF),
        v(chunks, BF), v(chunks, BF), v(chunks, BF),
        v(chunks, BF), v(chunks, BF),
        v(eight, BF), v(eight, BF), v(eight, BF), v(eight, BF),
        v((2, HIDP, ALL), F32),
        v((MP, 2 * QUART + 16, ALL), BF), v((MP, 2 * QUART + 16, ALL), BF),
        v((HIDP, ALL), BF),
        v((PK, 128), F32),
        sem((11,)), sem((5,)), sem((5, LINE)), sem((5,)), sem((5,)), sem((5, LINE)), sem((4, MP)),
    ]
    any_space = pl.BlockSpec(memory_space=pl.ANY)
    attended, layer = pl.pallas_call(
        kernel,
        out_shape=(jax.ShapeDtypeStruct((COL, TOK), BF), jax.ShapeDtypeStruct((COL, TOK), BF)),
        in_specs=[any_space] * 11,
        out_specs=(pl.BlockSpec(memory_space=pltpu.VMEM), pl.BlockSpec(memory_space=pltpu.VMEM)),
        scratch_shapes=scratch,
        compiler_params=pltpu.CompilerParams(
            collective_id=0, has_side_effects=True, vmem_limit_bytes=66700000
        ),
        name="layer",
    )(
        tokens, gain_attn.reshape(D // 128, 128), w_query.T, query_bias.reshape(1, COL), cache_keys, cache_values,
        w_out.T, gain_ffn.reshape(1, COL), w_gate.T, w_up.T, w_down,
    )
    return attended.T, layer.T


def solution(mesh):
    placed = (
        P("mp", None), P(), P(None, "seq"), P("seq"), P(None, "seq", None), P(None, "seq", None),
        P(None, "seq"), P("seq"), P("mp", "seq"), P("mp", "seq"), P("seq", "mp"),
    )
    return jax.shard_map(
        body, mesh=mesh, in_specs=placed, out_specs=(P("mp", "seq"), P("mp", "seq")), check_vma=False
    )
```

```python
import functools
import math

import jax
import jax.numpy as jnp
from jax import lax
from jax.experimental import pallas as pl
from jax.experimental.pallas import tpu as pltpu
from jax.sharding import PartitionSpec as P

D = 3584
HEAD = 128
GROUP = 7
KV = 4
CTX = 1024
SEQ = 64
MP = 4
TOK = 64
ALL = TOK * MP
COL = 56
FEAT = D // MP
PEER = FEAT // COL
HID = 296
QUART = 80
HIDP = QUART * MP
PK = 32
LINE = 8
EPS = 1e-06
MESH = pl.DeviceIdType.MESH
BF = jnp.bfloat16
F32 = jnp.float32
LOG2E = 1.0 / math.log(2.0)


def dot(a, b, dims=((1,), (0,))):
    return lax.dot_general(a, b, (dims, ((), ())), preferred_element_type=F32)


def low_lanes(rows):
    return lax.broadcasted_iota(jnp.int32, (rows, 128), 1) < 64


def row_ids(rows):
    return lax.broadcasted_iota(jnp.int32, (rows, 128), 0)


def swap(x):
    return pltpu.roll(x, 64, axis=1)


def column_of(row):
    n = row.shape[1]
    same = lax.broadcasted_iota(jnp.int32, (n, n), 0) == lax.broadcasted_iota(jnp.int32, (n, n), 1)
    return jnp.sum(jnp.where(same, jnp.broadcast_to(row, (n, n)), 0.0), axis=1, keepdims=True)


def split3(x):
    first = x.astype(BF).astype(F32)
    rest = x - first
    second = rest.astype(BF).astype(F32)
    return first, second, rest - second


def three_rows(x, rows, base=0):
    first, second, third = split3(x)
    at = lax.broadcasted_iota(jnp.int32, (rows, x.shape[1]), 0) - base
    return jnp.where(at == 0, first, jnp.where(at == 1, second, jnp.where(at == 2, third, 0.0)))


def merge(chunks, j):
    at = row_ids(8)
    high = jnp.logical_not(low_lanes(chunks.shape[0]))
    sides = ([], [])
    for i in range(chunks.shape[0]):
        part = chunks[i, 24:PK]
        sides[0].append(jnp.sum(jnp.where(at < 3, part, 0.0), axis=0, keepdims=True))
        sides[1].append(jnp.sum(jnp.where(jnp.logical_and(at >= 3, at < 6), part, 0.0), axis=0, keepdims=True))
    weights, levels = [], []
    for rows in sides:
        level = jnp.concatenate(rows, axis=0)
        level = jnp.where(high, level, swap(level))
        top = jnp.max(level, axis=0, keepdims=True)
        weight = jnp.exp2(level - top)
        total = jnp.sum(weight, axis=0, keepdims=True)
        weights.append(weight / total)
        levels.append(top + jnp.log(total) * LOG2E)
    edge = HEAD * ((j * COL) // HEAD + 1) - j * COL
    first_head = row_ids(PK) + jnp.where(low_lanes(PK), 0, PK) < edge
    acc = jnp.zeros((PK, 128), F32)
    for i in range(chunks.shape[0]):
        acc += chunks[i] * jnp.where(first_head, weights[0][i : i + 1], weights[1][i : i + 1])
    return acc, levels


def kernel(
    tokens_h, gain_attn_h, wq_h, bias_h, keys_h, values_h, wo_h, gain_ffn_h, wg_h, wu_h, wd_h,
    att_out, lay_out,
    tokens, gain_attn, wq, bias, keys, values, wo, gain_ffn, wg, wu, wd,
    normed, value_t, wd_t, hid_t, wo_e, work, outs, lsplit, stage2, stage6,
    own1, own4, held1, line3, held4, buf1, buf3, buf4, plane2, plane6, rel2, rel6, held2, held6,
    gu, gstage, gbuf, act, res,
    in_sem, zsend, zrecv, psend, precv, rrecv, asem,
):
    s = lax.axis_index("seq")
    m = lax.axis_index("mp")
    z, x, yh = lax.rem(s, LINE), lax.rem(s // LINE, 4), s // (4 * LINE)
    yl, c = m // 2, lax.rem(m, 2)
    line = s - z
    here = s // LINE
    xb = lax.rem(x, 2)
    own_j = LINE * xb + z
    mine = x // 2 == c
    same_y = yl == yh

    pairs = (
        (tokens_h, tokens), (gain_attn_h, gain_attn), (wq_h, wq), (bias_h, bias),
        (keys_h.at[m], keys), (values_h.at[m], values), (wo_h, wo), (gain_ffn_h, gain_ffn),
        (wg_h, wg), (wu_h, wu), (wd_h, wd.at[pl.ds(0, HID)]),
    )
    loads = [pltpu.make_async_copy(a, b, in_sem.at[i]) for i, (a, b) in enumerate(pairs)]
    for load in loads:
        load.start()

    bar = pltpu.get_barrier_semaphore()

    def greet(p, q):
        pl.semaphore_signal(bar, inc=1, device_id=(p, q), device_id_type=MESH)

    for i in range(1, 32):
        u, v, d = i // 16, (i // 8) % 2, i % 8
        greet(32 * lax.rem(yh + u, 2) + LINE * x + lax.rem(z + d, LINE), 2 * lax.rem(yl + v, 2) + c)
    for i in range(1, 8):
        greet(32 * yh + LINE * lax.rem(x + i % 4, 4) + z, 2 * yl + lax.rem(c + i // 4, 2))
    for i in range(1, 4):
        greet(32 * (1 - yh) + LINE * lax.rem(x + i, 4) + z, m)
    greet(s, 2 * (1 - yl) + 1 - c)

    loads[0].wait()
    loads[1].wait()
    normed[pl.ds(TOK, TOK), :] = jnp.zeros((TOK, D), BF)
    gain_row = jnp.concatenate([gain_attn[i : i + 1, :] for i in range(D // 128)], axis=1)

    def norm_rows(i, c):
        at = pl.multiple_of(i * 16, 16)
        x = tokens[pl.ds(at, 16), :].astype(F32)
        mean_sq = jnp.sum(x * x, axis=1, keepdims=True) * (1.0 / D)
        normed[pl.ds(at, 16), :] = (x * lax.rsqrt(mean_sq + EPS) * gain_row).astype(BF)
        return c

    lax.fori_loop(0, TOK // 16, norm_rows, 0)
    loads[2].wait()
    loads[3].wait()
    q_t = dot(wq[...], normed[...], ((1,), (1,))) + column_of(bias[...])
    low32 = low_lanes(PK)

    def packed(x):
        hi = jnp.concatenate([x[PK:COL], jnp.zeros((8, 128), F32)], axis=0)
        return jnp.where(low32, x[0:PK], swap(hi))

    def remote(src, dst, send_sem, recv_sem, p, q):
        pltpu.make_async_remote_copy(
            src_ref=src, dst_ref=dst, send_sem=send_sem, recv_sem=recv_sem, device_id=(p, q), device_id_type=MESH
        ).start()

    def copy(src, dst, send_sem, recv_sem, p, q, local):
        @pl.when(local)
        def _():
            pltpu.make_async_copy(src, dst, recv_sem).start()

        @pl.when(jnp.logical_not(local))
        def _():
            remote(src, dst, send_sem, recv_sem, p, q)

    def arrived(buf, sem):
        pltpu.make_async_copy(buf, buf, sem).wait()

    def near_first(i):
        return lax.rem(jnp.where(lax.rem(i, 2) == 1, (i + 1) // 2, LINE - i // 2), LINE)

    def far_first(i):
        return lax.rem(LINE + LINE // 2 + jnp.where(lax.rem(i, 2) == 1, -((i + 1) // 2), i // 2), LINE)

    def spread_yz(own, held, k):
        for d in (4, 3, 5, 2, 6, 1, 7, 0):
            for u in range(2):
                to = (32 * u + LINE * x + lax.rem(z + d, LINE), 2 * yh + c)
                sems = (zsend.at[k], zrecv.at[k, (LINE - d) % LINE])
                slot = held.at[2 * z + yl]
                if d:
                    remote(own, slot, *sems, *to)
                else:
                    copy(own, slot, *sems, *to, jnp.logical_and(yh == u, same_y))

    def spread_x(held, buf, k):
        def step(i, carry):
            e = near_first(i)
            pair = pl.ds(2 * lax.rem(z + e, LINE), 2)
            arrived(held.at[pair], zrecv.at[k, e])
            for o in (2, 1, 3, 0):
                to = (32 * yh + LINE * lax.rem(x + o, 4) + z, 2 * yl + x // 2)
                args = (held.at[pair], buf.at[2 * xb + c, pair], psend.at[k], precv.at[k], *to)
                if o:
                    remote(*args)
                else:
                    copy(*args, mine)
            return carry

        lax.fori_loop(0, LINE, step, 0)

    def along_line(held, k):
        for d in (4, 3, 5, 2, 6, 1, 7):
            remote(held.at[z], held.at[z], zsend.at[k], zrecv.at[k, LINE - d], line + lax.rem(z + d, LINE), m)

    def on_to_plane(held, buf, k):
        def step(i, carry):
            e = near_first(i)
            at = lax.rem(z + e, LINE)

            @pl.when(i > 0)
            def _():
                arrived(held.at[at], zrecv.at[k, e])

            for d in range(1, 8):
                p = LINE * lax.rem(here + d, 8) + z
                remote(held.at[at], buf.at[here, at], psend.at[k], precv.at[k], p, m)
            pltpu.make_async_copy(held.at[at], buf.at[here, at], precv.at[k]).start()
            return carry

        lax.fori_loop(0, LINE, step, 0)

    own1[...] = packed(q_t).astype(BF)

    loads[5].wait()
    value_t[...] = values[...].T
    first = lax.broadcasted_iota(jnp.int32, (COL, D), 1) - lax.broadcasted_iota(jnp.int32, (COL, D), 0)
    pick = jnp.where(first == s * COL, 1.0, 0.0).astype(BF)
    normed[pl.ds(0, TOK), :] = tokens[...]
    hid_t[...] = dot(pick, normed[...], ((1,), (1,)))
    loads[10].wait()
    wd[pl.ds(HID, HIDP - HID), :] = jnp.zeros((HIDP - HID, FEAT), BF)
    wd_t[...] = wd[...].T
    outs[pl.ds(FEAT, 8), :] = jnp.zeros((8, ALL), F32)
    gu[:, pl.ds(HID, HIDP - HID), :] = jnp.zeros((2, HIDP - HID, ALL), F32)
    wide = PEER * PK
    c_at = lax.broadcasted_iota(jnp.int32, (FEAT, wide), 1)
    r_at = lax.broadcasted_iota(jnp.int32, (FEAT, wide), 0) - COL * (c_at // PK)
    c_at = lax.rem(c_at, PK)
    pick_lo = jnp.where(r_at == c_at, 1.0, 0.0).astype(BF)
    pick_hi = jnp.where(jnp.logical_and(r_at == c_at + PK, c_at < COL - PK), 1.0, 0.0).astype(BF)
    wo_e[...] = jnp.zeros((128, SEQ * PK), BF)
    loads[6].wait()
    for i in range(MP):
        part = wo[:, pl.ds(i * FEAT, FEAT)]
        wo_e[pl.ds(0, COL), pl.ds(i * wide, wide)] = dot(part, pick_lo).astype(BF)
        wo_e[pl.ds(64, COL), pl.ds(i * wide, wide)] = dot(part, pick_hi).astype(BF)
    for i in (4, 7, 8, 9):
        loads[i].wait()

    pl.semaphore_wait(bar, 42)
    spread_yz(own1, held1, 0)
    spread_x(held1, buf1, 0)

    def unpack_chunks(buf, squares):
        def one(j, sums):
            sums = list(sums)
            for t in range(2):
                a = buf[2 * (j // LINE), 2 * lax.rem(j, LINE) + t].astype(F32)
                b = buf[2 * (j // LINE) + 1, 2 * lax.rem(j, LINE) + t].astype(F32)
                lo = jnp.where(low32, a, swap(b))
                hi = jnp.where(low32, swap(a), b)
                at = pl.multiple_of(j * COL, 8)
                work[pl.ds(at, PK), pl.ds(128 * t, 128)] = lo
                work[pl.ds(pl.multiple_of(at + PK, 8), COL - PK), pl.ds(128 * t, 128)] = hi[0 : COL - PK]
                if squares:
                    sums[t] = sums[t] + hi[COL - PK : PK]
            return tuple(sums)

        zero = jnp.zeros((8, 128), F32)
        return lax.fori_loop(0, PEER, one, (zero, zero), unroll=4)

    low8 = low_lanes(8)

    def collect_x(stage, plane, k, stats):
        def step(i, carry):
            e = far_first(i)
            to_z = lax.rem(z + e, LINE)
            for half in range(2):
                j = half * LINE + to_z
                at = pl.multiple_of(j * COL, 8)
                for t in range(2):
                    r = outs[pl.ds(at, 2 * PK), pl.ds(128 * t, 128)]
                    lo, hi = r[0:PK], r[PK : 2 * PK]
                    a = jnp.where(low32, lo, swap(hi))
                    b = jnp.where(low32, swap(lo), hi)
                    if stats:
                        h0, h1 = (j * COL) // HEAD, (j * COL + COL - 1) // HEAD
                        both = jnp.where(
                            row_ids(8) < 3, lsplit[h0, :, pl.ds(128 * t, 128)], lsplit[h1, :, pl.ds(128 * t, 128)]
                        )
                        a = jnp.concatenate([a[0:24], jnp.where(low8, a[24:PK], swap(both))], axis=0)
                        b = jnp.concatenate([b[0:24], jnp.where(low8, b[24:PK], both)], axis=0)
                    stage[to_z, 2 * half, t] = a.astype(BF)
                    stage[to_z, 2 * half + 1, t] = b.astype(BF)
            for g in range(4):
                to = (32 * yh + LINE * (2 * c + g // 2) + z, 2 * yl + g % 2)
                local = jnp.logical_and(2 * c + g // 2 == x, g % 2 == c)
                copy(stage.at[to_z, g], plane.at[to_z, x], psend.at[k], rrecv.at[k, e], *to, local)
            return carry

        lax.fori_loop(0, LINE, step, 0)

    def collect_yz(plane, rel, held, k, join):
        def step(i, carry):
            e = far_first(i)
            to_z = lax.rem(z + e, LINE)
            arrived(plane.at[to_z], rrecv.at[k, e])
            for t in range(2):
                rel[2 * to_z + t] = join(plane[to_z, :, t].astype(F32), to_z).astype(BF)
                local = jnp.logical_and(jnp.logical_and(same_y, e == 0), yl == t)
                to = (32 * yl + LINE * x + to_z, 2 * t + c)
                copy(rel.at[2 * to_z + t], held.at[2 * z + yh], zsend.at[k], zrecv.at[k, 0], *to, local)
            return carry

        lax.fori_loop(0, LINE, step, 0)
        arrived(held, zrecv.at[k, 0])

    arrived(buf1, precv.at[0])
    unpack_chunks(buf1, False)
    scale = HEAD ** (-0.5) * LOG2E

    def one_head(h, c):
        at = pl.multiple_of(h * HEAD, HEAD)
        scores = dot(keys[...], work[pl.ds(at, HEAD), :].astype(BF)) * scale
        top = jnp.max(scores, axis=0, keepdims=True)
        probs = jnp.exp2(scores - top)
        total = jnp.sum(probs, axis=0, keepdims=True)
        outs[pl.ds(at, HEAD), :] = dot(value_t[...], probs.astype(BF)) * (1.0 / total)
        level = top + jnp.log(total) * LOG2E
        lsplit[h] = three_rows(level, 8) + three_rows(level, 8, 3)
        return c

    lax.fori_loop(0, GROUP, one_head, 0)

    collect_x(stage2, plane2, 1, True)

    def join2(chunks, to_z):
        value, levels = merge(chunks, LINE * xb + to_z)
        rows = three_rows(levels[0], 8) + three_rows(levels[1], 8, 3)
        return jnp.concatenate([value[0:24], jnp.where(low8, value[24:PK], rows)], axis=0)

    collect_yz(plane2, rel2, held2, 1, join2)
    merged = merge(held2[...].astype(F32), own_j)[0].astype(BF)
    line3[z] = merged

    along_line(line3, 2)
    on_to_plane(line3, buf3, 2)

    def unpacked(x, out):
        out[pl.ds(0, PK), :] = x[:, 0:64].astype(BF)
        out[pl.ds(PK, COL - PK), :] = swap(x)[0 : COL - PK, 0:64].astype(BF)

    unpacked(merged.astype(F32), att_out)
    res_hid = packed(hid_t[...])
    gain_col = jnp.broadcast_to(column_of(gain_ffn[...]), (COL, 128))
    gain_pk = packed(gain_col)
    arrived(buf3, precv.at[2])
    both = dot(wo_e[...], buf3[...].reshape(SEQ * PK, 128))
    residual = res_hid + packed(both[0:COL] + swap(both[64 : 64 + COL]))
    res[...] = residual

    real = jnp.logical_or(low32, row_ids(PK) < COL - PK)
    squares = jnp.sum(jnp.where(real, residual * residual, 0.0), axis=0, keepdims=True)
    squares = squares + swap(squares)
    scaled = residual * gain_pk
    own4[...] = jnp.where(real, scaled, three_rows(squares, PK, 24)).astype(BF)
    spread_yz(own4, held4, 3)
    spread_x(held4, buf4, 3)
    arrived(buf4, precv.at[3])
    sums = unpack_chunks(buf4, True)
    sq = jnp.concatenate([jnp.sum(x, axis=0, keepdims=True) for x in sums], axis=1)

    features = work[pl.ds(0, FEAT), :].astype(BF)
    gu[0, pl.ds(0, HID), :] = dot(wg[...], features)
    gu[1, pl.ds(0, HID), :] = dot(wu[...], features)
    sq_rows = three_rows(sq, 16).astype(BF)
    for d in range(1, MP):
        q = lax.rem(m + d, MP)
        at = pl.multiple_of(q * QUART, 16)
        gstage[d, pl.ds(0, QUART), :] = gu[0, pl.ds(at, QUART), :].astype(BF)
        gstage[d, pl.ds(QUART, QUART), :] = gu[1, pl.ds(at, QUART), :].astype(BF)
        gstage[d, pl.ds(2 * QUART, 16), :] = sq_rows
        pltpu.make_async_remote_copy(
            src_ref=gstage.at[d], dst_ref=gbuf.at[d], send_sem=asem.at[0, d], recv_sem=asem.at[1, d],
            device_id=(s, q), device_id_type=MESH,
        ).start()
    at = pl.multiple_of(m * QUART, 16)
    gate = gu[0, pl.ds(at, QUART), :]
    up = gu[1, pl.ds(at, QUART), :]
    for d in range(1, MP):
        arrived(gbuf.at[d], asem.at[1, d])
        gate += gbuf[d, pl.ds(0, QUART), :].astype(F32)
        up += gbuf[d, pl.ds(QUART, QUART), :].astype(F32)
        sq += jnp.sum(gbuf[d, pl.ds(2 * QUART, 16), :].astype(F32), axis=0, keepdims=True)
    factor = lax.rsqrt(sq * (1.0 / D) + EPS)
    gate = gate * factor
    up = up * factor
    act[pl.ds(at, QUART), :] = (gate / (1.0 + jnp.exp(-gate)) * up).astype(BF)
    for d in range(1, MP):
        q = lax.rem(m + d, MP)
        pltpu.make_async_remote_copy(
            src_ref=act.at[pl.ds(at, QUART)], dst_ref=act.at[pl.ds(at, QUART)],
            send_sem=asem.at[2, d], recv_sem=asem.at[3, d], device_id=(s, q), device_id_type=MESH,
        ).start()
    for d in range(1, MP):
        arrived(act.at[pl.ds(pl.multiple_of(lax.rem(m + MP - d, MP) * QUART, 16), QUART)], asem.at[3, d])

    outs[pl.ds(0, FEAT), :] = dot(wd_t[...], act[...])
    collect_x(stage6, plane6, 4, False)
    collect_yz(plane6, rel6, held6, 4, lambda chunks, to_z: jnp.sum(chunks, axis=0))
    unpacked(res[...] + jnp.sum(held6[...].astype(F32), axis=0), lay_out)

    for k, buf in ((0, buf1), (1, stage2), (3, buf4), (4, stage6)):
        for own, some, sem in ((same_y, held1.at[pl.ds(0, 15)], zsend.at[k]), (mine, None, psend.at[k])):
            whole = held1 if some is not None else buf
            part = some
            if part is None:
                part = buf.at[pl.ds(0, 3)] if buf.shape[0] == 4 else buf.at[pl.ds(0, 6)]

            @pl.when(own)
            def _(part=part, sem=sem):
                arrived(part, sem)

            @pl.when(jnp.logical_not(own))
            def _(whole=whole, sem=sem):
                arrived(whole, sem)

    arrived(line3.at[pl.ds(0, 7)], zsend.at[2])
    arrived(buf3.at[pl.ds(0, 7)], psend.at[2])
    for d in range(1, MP):
        arrived(gstage.at[d], asem.at[0, d])
        arrived(act.at[pl.ds(at, QUART)], asem.at[2, d])


def body(tokens, gain_attn, w_query, query_bias, cache_keys, cache_values, w_out, gain_ffn, w_gate, w_up, w_down):
    v = pltpu.VMEM
    one, eight, pairs = (PK, 128), (LINE, PK, 128), (2 * LINE, PK, 128)
    chunks, users, owners = (8, LINE, PK, 128), (4, 2 * LINE, PK, 128), (LINE, 4, 2, PK, 128)
    sem = pltpu.SemaphoreType.DMA
    scratch = [
        v((TOK, D), BF), v((D // 128, 128), F32), v((COL, D), BF), v((1, COL), F32), v((CTX, HEAD), BF),
        v((CTX, HEAD), BF), v((COL, D), BF), v((1, COL), F32), v((HID, FEAT), BF), v((HID, FEAT), BF),
        v((HIDP, FEAT), BF),
        v((2 * TOK, D), BF),
        v((HEAD, CTX), BF),
        v((FEAT, HIDP), BF),
        v((COL, 128), F32),
        v((128, SEQ * PK), BF),
        v((FEAT, ALL), F32),
        v((FEAT + 8, ALL), F32),
        v((8, 8, ALL), F32),
        v(owners, BF), v(owners, BF),
        v(one, BF), v(one, BF), v(pairs, BF), v(eight, BF), v(pairs, BF),
        v(users, BF), v(chunks, BF), v(users, BF),
        v(owners, BF), v(owners, BF),
        v(pairs, BF), v(pairs, BF), v(pairs, BF), v(pairs, BF),
        v((2, HIDP, ALL), F32),
        v((MP, 2 * QUART + 16, ALL), BF), v((MP, 2 * QUART + 16, ALL), BF),
        v((HIDP, ALL), BF),
        v((PK, 128), F32),
        sem((11,)), sem((5,)), sem((5, LINE)), sem((5,)), sem((5,)), sem((5, LINE)), sem((4, MP)),
    ]
    any_space = pl.BlockSpec(memory_space=pl.ANY)
    attended, layer = pl.pallas_call(
        kernel,
        out_shape=(jax.ShapeDtypeStruct((COL, TOK), BF), jax.ShapeDtypeStruct((COL, TOK), BF)),
        in_specs=[any_space] * 11,
        out_specs=(pl.BlockSpec(memory_space=pltpu.VMEM), pl.BlockSpec(memory_space=pltpu.VMEM)),
        scratch_shapes=scratch,
        compiler_params=pltpu.CompilerParams(
            collective_id=0, has_side_effects=True, vmem_limit_bytes=66700000
        ),
        name="layer",
    )(
        tokens, gain_attn.reshape(D // 128, 128), w_query.T, query_bias.reshape(1, COL), cache_keys, cache_values,
        w_out.T, gain_ffn.reshape(1, COL), w_gate.T, w_up.T, w_down,
    )
    return attended.T, layer.T


def solution(mesh):
    placed = (
        P("mp", None), P(), P(None, "seq"), P("seq"), P(None, "seq", None), P(None, "seq", None),
        P(None, "seq"), P("seq"), P("mp", "seq"), P("mp", "seq"), P("seq", "mp"),
    )
    return jax.shard_map(
        body, mesh=mesh, in_specs=placed, out_specs=(P("mp", "seq"), P("mp", "seq")), check_vma=False
    )
```

```python
import functools
import math

import jax
import jax.numpy as jnp
from jax import lax
from jax.experimental import pallas as pl
from jax.experimental.pallas import tpu as pltpu
from jax.sharding import PartitionSpec as P

D = 3584
HEAD = 128
GROUP = 7
KV = 4
CTX = 1024
SEQ = 64
MP = 4
TOK = 64
ALL = TOK * MP
COL = 56
FEAT = D // MP
PEER = FEAT // COL
HID = 296
QUART = 80
HIDP = QUART * MP
PK = 32
LINE = 8
EPS = 1e-06
MESH = pl.DeviceIdType.MESH
BF = jnp.bfloat16
F32 = jnp.float32
LOG2E = 1.0 / math.log(2.0)


def dot(a, b, dims=((1,), (0,))):
    return lax.dot_general(a, b, (dims, ((), ())), preferred_element_type=F32)


def low_lanes(rows):
    return lax.broadcasted_iota(jnp.int32, (rows, 128), 1) < 64


def row_ids(rows):
    return lax.broadcasted_iota(jnp.int32, (rows, 128), 0)


def swap(x):
    return pltpu.roll(x, 64, axis=1)


def column_of(row):
    n = row.shape[1]
    same = lax.broadcasted_iota(jnp.int32, (n, n), 0) == lax.broadcasted_iota(jnp.int32, (n, n), 1)
    return jnp.sum(jnp.where(same, jnp.broadcast_to(row, (n, n)), 0.0), axis=1, keepdims=True)


def split3(x):
    first = x.astype(BF).astype(F32)
    rest = x - first
    second = rest.astype(BF).astype(F32)
    return first, second, rest - second


def three_rows(x, rows, base=0):
    first, second, third = split3(x)
    at = lax.broadcasted_iota(jnp.int32, (rows, x.shape[1]), 0) - base
    return jnp.where(at == 0, first, jnp.where(at == 1, second, jnp.where(at == 2, third, 0.0)))


def merge(chunks, j):
    at = row_ids(8)
    high = jnp.logical_not(low_lanes(chunks.shape[0]))
    sides = ([], [])
    for i in range(chunks.shape[0]):
        part = chunks[i, 24:PK]
        sides[0].append(jnp.sum(jnp.where(at < 3, part, 0.0), axis=0, keepdims=True))
        sides[1].append(jnp.sum(jnp.where(jnp.logical_and(at >= 3, at < 6), part, 0.0), axis=0, keepdims=True))
    weights, levels = [], []
    for rows in sides:
        level = jnp.concatenate(rows, axis=0)
        level = jnp.where(high, level, swap(level))
        top = jnp.max(level, axis=0, keepdims=True)
        weight = jnp.exp2(level - top)
        total = jnp.sum(weight, axis=0, keepdims=True)
        weights.append(weight / total)
        levels.append(top + jnp.log(total) * LOG2E)
    edge = HEAD * ((j * COL) // HEAD + 1) - j * COL
    first_head = row_ids(PK) + jnp.where(low_lanes(PK), 0, PK) < edge
    acc = jnp.zeros((PK, 128), F32)
    for i in range(chunks.shape[0]):
        acc += chunks[i] * jnp.where(first_head, weights[0][i : i + 1], weights[1][i : i + 1])
    return acc, levels


def kernel(
    tokens_h, gain_attn_h, wq_h, bias_h, keys_h, values_h, wo_h, gain_ffn_h, wg_h, wu_h, wd_h,
    att_out, lay_out,
    tokens, gain_attn, wq, bias, keys, values, wo, gain_ffn, wg, wu, wd,
    normed, value_t, wd_t, hid_t, wo_e, work, outs, lsplit, stage2, stage6,
    own1, own4, held1, line3, held4, buf1, buf3, buf4, plane2, plane6, rel2, rel6, held2, held6,
    gu, gstage, gbuf, act, res,
    in_sem, zsend, zrecv, psend, precv, rrecv, asem,
):
    s = lax.axis_index("seq")
    m = lax.axis_index("mp")
    z, x, yh = lax.rem(s, LINE), lax.rem(s // LINE, 4), s // (4 * LINE)
    yl, c = m // 2, lax.rem(m, 2)
    line = s - z
    here = s // LINE
    xb = lax.rem(x, 2)
    own_j = LINE * xb + z
    mine = x // 2 == c
    same_y = yl == yh

    pairs = (
        (tokens_h, tokens), (gain_attn_h, gain_attn), (wq_h, wq), (bias_h, bias),
        (keys_h.at[m], keys), (values_h.at[m], values), (wo_h, wo), (gain_ffn_h, gain_ffn),
        (wg_h, wg), (wu_h, wu), (wd_h, wd.at[pl.ds(0, HID)]),
    )
    loads = [pltpu.make_async_copy(a, b, in_sem.at[i]) for i, (a, b) in enumerate(pairs)]
    for load in loads:
        load.start()

    bar = pltpu.get_barrier_semaphore()

    def greet(p, q):
        pl.semaphore_signal(bar, inc=1, device_id=(p, q), device_id_type=MESH)

    for i in range(1, 32):
        u, v, d = i // 16, (i // 8) % 2, i % 8
        greet(32 * lax.rem(yh + u, 2) + LINE * x + lax.rem(z + d, LINE), 2 * lax.rem(yl + v, 2) + c)
    for i in range(1, 8):
        greet(32 * yh + LINE * lax.rem(x + i % 4, 4) + z, 2 * yl + lax.rem(c + i // 4, 2))
    for i in range(1, 4):
        greet(32 * (1 - yh) + LINE * lax.rem(x + i, 4) + z, m)
    greet(s, 2 * (1 - yl) + 1 - c)

    loads[0].wait()
    loads[1].wait()
    normed[pl.ds(TOK, TOK), :] = jnp.zeros((TOK, D), BF)
    gain_row = jnp.concatenate([gain_attn[i : i + 1, :] for i in range(D // 128)], axis=1)

    def norm_rows(i, c):
        at = pl.multiple_of(i * 16, 16)
        x = tokens[pl.ds(at, 16), :].astype(F32)
        mean_sq = jnp.sum(x * x, axis=1, keepdims=True) * (1.0 / D)
        normed[pl.ds(at, 16), :] = (x * lax.rsqrt(mean_sq + EPS) * gain_row).astype(BF)
        return c

    lax.fori_loop(0, TOK // 16, norm_rows, 0)
    loads[2].wait()
    loads[3].wait()
    q_t = dot(wq[...], normed[...], ((1,), (1,))) + column_of(bias[...])
    low32 = low_lanes(PK)

    def packed(x):
        hi = jnp.concatenate([x[PK:COL], jnp.zeros((8, 128), F32)], axis=0)
        return jnp.where(low32, x[0:PK], swap(hi))

    def remote(src, dst, send_sem, recv_sem, p, q):
        pltpu.make_async_remote_copy(
            src_ref=src, dst_ref=dst, send_sem=send_sem, recv_sem=recv_sem, device_id=(p, q), device_id_type=MESH
        ).start()

    def copy(src, dst, send_sem, recv_sem, p, q, local):
        @pl.when(local)
        def _():
            pltpu.make_async_copy(src, dst, recv_sem).start()

        @pl.when(jnp.logical_not(local))
        def _():
            remote(src, dst, send_sem, recv_sem, p, q)

    def arrived(buf, sem):
        pltpu.make_async_copy(buf, buf, sem).wait()

    def near_first(i):
        return lax.rem(jnp.where(lax.rem(i, 2) == 1, (i + 1) // 2, LINE - i // 2), LINE)

    def far_first(i):
        return lax.rem(LINE + LINE // 2 + jnp.where(lax.rem(i, 2) == 1, -((i + 1) // 2), i // 2), LINE)

    def spread_yz(own, held, k):
        for d in (4, 3, 5, 2, 6, 1, 7, 0):
            for u in range(2):
                to = (32 * u + LINE * x + lax.rem(z + d, LINE), 2 * yh + c)
                sems = (zsend.at[k], zrecv.at[k, yl, (LINE - d) % LINE])
                slot = held.at[yl, z]
                if d:
                    remote(own, slot, *sems, *to)
                else:
                    copy(own, slot, *sems, *to, jnp.logical_and(yh == u, same_y))

    def spread_x(held, buf, k):
        for t in range(2):

            def step(i, carry, t=t):
                e = near_first(i)
                at = lax.rem(z + e, LINE)
                arrived(held.at[t, at], zrecv.at[k, t, e])
                for o in (2, 1, 3, 0):
                    to = (32 * yh + LINE * lax.rem(x + o, 4) + z, 2 * yl + x // 2)
                    args = (held.at[t, at], buf.at[t, 2 * xb + c, at], psend.at[k], precv.at[k, t], *to)
                    if o:
                        remote(*args)
                    else:
                        copy(*args, mine)
                return carry

            lax.fori_loop(0, LINE, step, 0)

    def along_line(held, k):
        for d in (4, 3, 5, 2, 6, 1, 7):
            remote(held.at[z], held.at[z], zsend.at[k], zrecv.at[k, 0, LINE - d], line + lax.rem(z + d, LINE), m)

    def on_to_plane(held, buf, k):
        def step(i, carry):
            e = near_first(i)
            at = lax.rem(z + e, LINE)

            @pl.when(i > 0)
            def _():
                arrived(held.at[at], zrecv.at[k, 0, e])

            for d in range(1, 8):
                p = LINE * lax.rem(here + d, 8) + z
                remote(held.at[at], buf.at[here, at], psend.at[k], precv.at[k, 0], p, m)
            pltpu.make_async_copy(held.at[at], buf.at[here, at], precv.at[k, 0]).start()
            return carry

        lax.fori_loop(0, LINE, step, 0)

    own1[...] = packed(q_t).astype(BF)

    loads[5].wait()
    value_t[...] = values[...].T
    first = lax.broadcasted_iota(jnp.int32, (COL, D), 1) - lax.broadcasted_iota(jnp.int32, (COL, D), 0)
    pick = jnp.where(first == s * COL, 1.0, 0.0).astype(BF)
    normed[pl.ds(0, TOK), :] = tokens[...]
    hid_t[...] = dot(pick, normed[...], ((1,), (1,)))
    loads[10].wait()
    wd[pl.ds(HID, HIDP - HID), :] = jnp.zeros((HIDP - HID, FEAT), BF)
    wd_t[...] = wd[...].T
    outs[pl.ds(FEAT, 8), :] = jnp.zeros((8, ALL), F32)
    gu[:, pl.ds(HID, HIDP - HID), :] = jnp.zeros((2, HIDP - HID, ALL), F32)
    wide = PEER * PK
    c_at = lax.broadcasted_iota(jnp.int32, (FEAT, wide), 1)
    r_at = lax.broadcasted_iota(jnp.int32, (FEAT, wide), 0) - COL * (c_at // PK)
    c_at = lax.rem(c_at, PK)
    pick_lo = jnp.where(r_at == c_at, 1.0, 0.0).astype(BF)
    pick_hi = jnp.where(jnp.logical_and(r_at == c_at + PK, c_at < COL - PK), 1.0, 0.0).astype(BF)
    wo_e[...] = jnp.zeros((128, SEQ * PK), BF)
    loads[6].wait()
    for i in range(MP):
        part = wo[:, pl.ds(i * FEAT, FEAT)]
        wo_e[pl.ds(0, COL), pl.ds(i * wide, wide)] = dot(part, pick_lo).astype(BF)
        wo_e[pl.ds(64, COL), pl.ds(i * wide, wide)] = dot(part, pick_hi).astype(BF)
    for i in (4, 7, 8, 9):
        loads[i].wait()

    pl.semaphore_wait(bar, 42)
    spread_yz(own1, held1, 0)
    spread_x(held1, buf1, 0)

    def unpack_chunks(buf, t, squares):
        tile = pl.ds(128 * t, 128)

        def one(j, total):
            a = buf[t, 2 * (j // LINE), lax.rem(j, LINE)].astype(F32)
            b = buf[t, 2 * (j // LINE) + 1, lax.rem(j, LINE)].astype(F32)
            lo = jnp.where(low32, a, swap(b))
            hi = jnp.where(low32, swap(a), b)
            at = pl.multiple_of(j * COL, 8)
            work[pl.ds(at, PK), tile] = lo
            work[pl.ds(pl.multiple_of(at + PK, 8), COL - PK), tile] = hi[0 : COL - PK]
            return total + hi[COL - PK : PK] if squares else total

        return lax.fori_loop(0, PEER, one, jnp.zeros((8, 128), F32), unroll=4)

    low8 = low_lanes(8)

    def collect_x(stage, plane, k, t, stats):
        tile = pl.ds(128 * t, 128)

        def step(i, carry):
            e = far_first(i)
            to_z = lax.rem(z + e, LINE)
            for half in range(2):
                j = half * LINE + to_z
                r = outs[pl.ds(pl.multiple_of(j * COL, 8), 2 * PK), tile]
                lo, hi = r[0:PK], r[PK : 2 * PK]
                a = jnp.where(low32, lo, swap(hi))
                b = jnp.where(low32, swap(lo), hi)
                if stats:
                    h0, h1 = (j * COL) // HEAD, (j * COL + COL - 1) // HEAD
                    both = jnp.where(row_ids(8) < 3, lsplit[h0, :, tile], lsplit[h1, :, tile])
                    a = jnp.concatenate([a[0:24], jnp.where(low8, a[24:PK], swap(both))], axis=0)
                    b = jnp.concatenate([b[0:24], jnp.where(low8, b[24:PK], both)], axis=0)
                stage[t, to_z, 2 * half] = a.astype(BF)
                stage[t, to_z, 2 * half + 1] = b.astype(BF)
            for g in range(4):
                to = (32 * yh + LINE * (2 * c + g // 2) + z, 2 * yl + g % 2)
                local = jnp.logical_and(2 * c + g // 2 == x, g % 2 == c)
                copy(stage.at[t, to_z, g], plane.at[t, to_z, x], psend.at[k], rrecv.at[k, t, e], *to, local)
            return carry

        lax.fori_loop(0, LINE, step, 0)

    def collect_yz(plane, rel, held, k, join):
        for t in range(2):

            def step(i, carry, t=t):
                e = far_first(i)
                to_z = lax.rem(z + e, LINE)
                arrived(plane.at[t, to_z], rrecv.at[k, t, e])
                rel[t, to_z] = join(plane[t, to_z].astype(F32), to_z).astype(BF)
                local = jnp.logical_and(jnp.logical_and(same_y, e == 0), yl == t)
                to = (32 * yl + LINE * x + to_z, 2 * t + c)
                copy(rel.at[t, to_z], held.at[2 * z + yh], zsend.at[k], zrecv.at[k, 0, 0], *to, local)
                return carry

            lax.fori_loop(0, LINE, step, 0)
        arrived(held, zrecv.at[k, 0, 0])

    scale = HEAD ** (-0.5) * LOG2E

    def attend(t, h, n):
        tile = pl.ds(128 * t, 128)
        rows = [pl.ds(pl.multiple_of((h + i) * HEAD, HEAD), HEAD) for i in range(n)]
        queries = jnp.concatenate([work[r, tile].astype(BF) for r in rows], axis=1)
        scores = dot(keys[...], queries) * scale
        top = jnp.max(scores, axis=0, keepdims=True)
        probs = jnp.exp2(scores - top)
        total = jnp.sum(probs, axis=0, keepdims=True)
        value = dot(value_t[...], probs.astype(BF)) * (1.0 / total)
        level = top + jnp.log(total) * LOG2E
        parts = three_rows(level, 8) + three_rows(level, 8, 3)
        for i in range(n):
            outs[rows[i], tile] = value[:, 128 * i : 128 * (i + 1)]
            lsplit[h + i, :, tile] = parts[:, 128 * i : 128 * (i + 1)]

    for t in range(2):
        arrived(buf1.at[t], precv.at[0, t])
        unpack_chunks(buf1, t, False)

        def two_heads(i, carry, t=t):
            attend(t, 2 * i, 2)
            return carry

        lax.fori_loop(0, GROUP // 2, two_heads, 0)
        attend(t, GROUP - 1, 1)
        collect_x(stage2, plane2, 1, t, True)

    def join2(chunks, to_z):
        value, levels = merge(chunks, LINE * xb + to_z)
        rows = three_rows(levels[0], 8) + three_rows(levels[1], 8, 3)
        return jnp.concatenate([value[0:24], jnp.where(low8, value[24:PK], rows)], axis=0)

    collect_yz(plane2, rel2, held2, 1, join2)
    merged = merge(held2[...].astype(F32), own_j)[0].astype(BF)
    line3[z] = merged

    along_line(line3, 2)
    on_to_plane(line3, buf3, 2)

    def unpacked(x, out):
        out[pl.ds(0, PK), :] = x[:, 0:64].astype(BF)
        out[pl.ds(PK, COL - PK), :] = swap(x)[0 : COL - PK, 0:64].astype(BF)

    unpacked(merged.astype(F32), att_out)
    res_hid = packed(hid_t[...])
    gain_col = jnp.broadcast_to(column_of(gain_ffn[...]), (COL, 128))
    gain_pk = packed(gain_col)
    arrived(buf3, precv.at[2, 0])
    both = dot(wo_e[...], buf3[...].reshape(SEQ * PK, 128))
    residual = res_hid + packed(both[0:COL] + swap(both[64 : 64 + COL]))
    res[...] = residual

    real = jnp.logical_or(low32, row_ids(PK) < COL - PK)
    squares = jnp.sum(jnp.where(real, residual * residual, 0.0), axis=0, keepdims=True)
    squares = squares + swap(squares)
    scaled = residual * gain_pk
    own4[...] = jnp.where(real, scaled, three_rows(squares, PK, 24)).astype(BF)
    spread_yz(own4, held4, 3)
    spread_x(held4, buf4, 3)

    sqs = []
    for t in range(2):
        tile = pl.ds(128 * t, 128)
        arrived(buf4.at[t], precv.at[3, t])
        sq = jnp.sum(unpack_chunks(buf4, t, True), axis=0, keepdims=True)
        features = work[pl.ds(0, FEAT), tile].astype(BF)
        gu[0, pl.ds(0, HID), tile] = dot(wg[...], features)
        gu[1, pl.ds(0, HID), tile] = dot(wu[...], features)
        sq_rows = three_rows(sq, 16).astype(BF)
        for d in (2, 3, 1):
            q = lax.rem(m + d, MP)
            at = pl.multiple_of(q * QUART, 16)
            gstage[t, d, pl.ds(0, QUART)] = gu[0, pl.ds(at, QUART), tile].astype(BF)
            gstage[t, d, pl.ds(QUART, QUART)] = gu[1, pl.ds(at, QUART), tile].astype(BF)
            gstage[t, d, pl.ds(2 * QUART, 16)] = sq_rows
            remote(gstage.at[t, d], gbuf.at[t, d], asem.at[0, t, d], asem.at[1, t, d], s, q)
        sqs.append(sq)
    at = pl.multiple_of(m * QUART, 16)
    own_rows = pl.ds(at, QUART)
    for t in range(2):
        tile = pl.ds(128 * t, 128)
        gate, up, sq = gu[0, own_rows, tile], gu[1, own_rows, tile], sqs[t]
        for d in (1, 3, 2):
            arrived(gbuf.at[t, d], asem.at[1, t, d])
            gate += gbuf[t, d, pl.ds(0, QUART)].astype(F32)
            up += gbuf[t, d, pl.ds(QUART, QUART)].astype(F32)
            sq += jnp.sum(gbuf[t, d, pl.ds(2 * QUART, 16)].astype(F32), axis=0, keepdims=True)
        factor = lax.rsqrt(sq * (1.0 / D) + EPS)
        gate = gate * factor
        up = up * factor
        act[t, own_rows] = (gate / (1.0 + jnp.exp(-gate)) * up).astype(BF)
        for d in (2, 3, 1):
            part = act.at[t, own_rows]
            remote(part, part, asem.at[2, t, d], asem.at[3, t, d], s, lax.rem(m + d, MP))

    for t in range(2):
        for d in (1, 3, 2):
            rows = pl.ds(pl.multiple_of(lax.rem(m + MP - d, MP) * QUART, 16), QUART)
            arrived(act.at[t, rows], asem.at[3, t, d])
        outs[pl.ds(0, FEAT), pl.ds(128 * t, 128)] = dot(wd_t[...], act[t])
        collect_x(stage6, plane6, 4, t, False)
    collect_yz(plane6, rel6, held6, 4, lambda chunks, to_z: jnp.sum(chunks, axis=0))
    unpacked(res[...] + jnp.sum(held6[...].astype(F32), axis=0), lay_out)

    fifteen, most = held2.at[pl.ds(0, 15)], buf3.at[pl.ds(0, 6)]
    for k in (0, 1, 3, 4):
        for own, part, whole, sem in ((same_y, fifteen, held2, zsend.at[k]), (mine, most, buf3, psend.at[k])):

            @pl.when(own)
            def _(part=part, sem=sem):
                arrived(part, sem)

            @pl.when(jnp.logical_not(own))
            def _(whole=whole, sem=sem):
                arrived(whole, sem)

    arrived(line3.at[pl.ds(0, 7)], zsend.at[2])
    arrived(buf3.at[pl.ds(0, 7)], psend.at[2])
    for t in range(2):
        for d in range(1, MP):
            arrived(gstage.at[t, d], asem.at[0, t, d])
            arrived(act.at[t, own_rows], asem.at[2, t, d])


def body(tokens, gain_attn, w_query, query_bias, cache_keys, cache_values, w_out, gain_ffn, w_gate, w_up, w_down):
    v = pltpu.VMEM
    one, eight, pairs, halves = (PK, 128), (LINE, PK, 128), (2 * LINE, PK, 128), (2, LINE, PK, 128)
    chunks, users, owners = (8, LINE, PK, 128), (2, 4, LINE, PK, 128), (2, LINE, 4, PK, 128)
    sem = pltpu.SemaphoreType.DMA
    scratch = [
        v((TOK, D), BF), v((D // 128, 128), F32), v((COL, D), BF), v((1, COL), F32), v((CTX, HEAD), BF),
        v((CTX, HEAD), BF), v((COL, D), BF), v((1, COL), F32), v((HID, FEAT), BF), v((HID, FEAT), BF),
        v((HIDP, FEAT), BF),
        v((2 * TOK, D), BF),
        v((HEAD, CTX), BF),
        v((FEAT, HIDP), BF),
        v((COL, 128), F32),
        v((128, SEQ * PK), BF),
        v((FEAT, ALL), F32),
        v((FEAT + 8, ALL), F32),
        v((8, 8, ALL), F32),
        v(owners, BF), v(owners, BF),
        v(one, BF), v(one, BF), v(halves, BF), v(eight, BF), v(halves, BF),
        v(users, BF), v(chunks, BF), v(users, BF),
        v(owners, BF), v(owners, BF),
        v(halves, BF), v(halves, BF), v(pairs, BF), v(pairs, BF),
        v((2, HIDP, ALL), F32),
        v((2, MP, 2 * QUART + 16, 128), BF), v((2, MP, 2 * QUART + 16, 128), BF),
        v((2, HIDP, 128), BF),
        v((PK, 128), F32),
        sem((11,)), sem((5,)), sem((5, 2, LINE)), sem((5,)), sem((5, 2)), sem((5, 2, LINE)), sem((4, 2, MP)),
    ]
    any_space = pl.BlockSpec(memory_space=pl.ANY)
    attended, layer = pl.pallas_call(
        kernel,
        out_shape=(jax.ShapeDtypeStruct((COL, TOK), BF), jax.ShapeDtypeStruct((COL, TOK), BF)),
        in_specs=[any_space] * 11,
        out_specs=(pl.BlockSpec(memory_space=pltpu.VMEM), pl.BlockSpec(memory_space=pltpu.VMEM)),
        scratch_shapes=scratch,
        compiler_params=pltpu.CompilerParams(
            collective_id=0, has_side_effects=True, vmem_limit_bytes=66700000
        ),
        name="layer",
    )(
        tokens, gain_attn.reshape(D // 128, 128), w_query.T, query_bias.reshape(1, COL), cache_keys, cache_values,
        w_out.T, gain_ffn.reshape(1, COL), w_gate.T, w_up.T, w_down,
    )
    return attended.T, layer.T


def solution(mesh):
    placed = (
        P("mp", None), P(), P(None, "seq"), P("seq"), P(None, "seq", None), P(None, "seq", None),
        P(None, "seq"), P("seq"), P("mp", "seq"), P("mp", "seq"), P("seq", "mp"),
    )
    return jax.shard_map(
        body, mesh=mesh, in_specs=placed, out_specs=(P("mp", "seq"), P("mp", "seq")), check_vma=False
    )
```

```python
import functools
import math

import jax
import jax.numpy as jnp
from jax import lax
from jax.experimental import pallas as pl
from jax.experimental.pallas import tpu as pltpu
from jax.sharding import PartitionSpec as P

D = 3584
HEAD = 128
GROUP = 7
KV = 4
CTX = 1024
SEQ = 64
MP = 4
TOK = 64
ALL = TOK * MP
COL = 56
FEAT = D // MP
PEER = FEAT // COL
HID = 296
SHARE = 160
HIDP = 2 * SHARE
PK = 32
LINE = 8
EPS = 1e-06
MESH = pl.DeviceIdType.MESH
BF = jnp.bfloat16
F32 = jnp.float32
LOG2E = 1.0 / math.log(2.0)


def dot(a, b, dims=((1,), (0,))):
    return lax.dot_general(a, b, (dims, ((), ())), preferred_element_type=F32)


def low_lanes(rows):
    return lax.broadcasted_iota(jnp.int32, (rows, 128), 1) < 64


def row_ids(rows):
    return lax.broadcasted_iota(jnp.int32, (rows, 128), 0)


def swap(x):
    return pltpu.roll(x, 64, axis=1)


def column_of(row):
    n = row.shape[1]
    same = lax.broadcasted_iota(jnp.int32, (n, n), 0) == lax.broadcasted_iota(jnp.int32, (n, n), 1)
    return jnp.sum(jnp.where(same, jnp.broadcast_to(row, (n, n)), 0.0), axis=1, keepdims=True)


def split3(x):
    first = x.astype(BF).astype(F32)
    rest = x - first
    second = rest.astype(BF).astype(F32)
    return first, second, rest - second


def three_rows(x, rows, base=0):
    first, second, third = split3(x)
    at = lax.broadcasted_iota(jnp.int32, (rows, x.shape[1]), 0) - base
    return jnp.where(at == 0, first, jnp.where(at == 1, second, jnp.where(at == 2, third, 0.0)))


def merge(chunks, j):
    at = row_ids(8)
    high = jnp.logical_not(low_lanes(chunks.shape[0]))
    sides = ([], [])
    for i in range(chunks.shape[0]):
        part = chunks[i, 24:PK]
        sides[0].append(jnp.sum(jnp.where(at < 3, part, 0.0), axis=0, keepdims=True))
        sides[1].append(jnp.sum(jnp.where(jnp.logical_and(at >= 3, at < 6), part, 0.0), axis=0, keepdims=True))
    weights, levels = [], []
    for rows in sides:
        level = jnp.concatenate(rows, axis=0)
        level = jnp.where(high, level, swap(level))
        top = jnp.max(level, axis=0, keepdims=True)
        weight = jnp.exp2(level - top)
        total = jnp.sum(weight, axis=0, keepdims=True)
        weights.append(weight / total)
        levels.append(top + jnp.log(total) * LOG2E)
    edge = HEAD * ((j * COL) // HEAD + 1) - j * COL
    first_head = row_ids(PK) + jnp.where(low_lanes(PK), 0, PK) < edge
    acc = jnp.zeros((PK, 128), F32)
    for i in range(chunks.shape[0]):
        acc += chunks[i] * jnp.where(first_head, weights[0][i : i + 1], weights[1][i : i + 1])
    return acc, levels


def kernel(
    tokens_h, gain_attn_h, wq_h, bias_h, keys_h, values_h, wo_h, gain_ffn_h, wg_h, wu_h, wd_h,
    att_out, lay_out,
    tokens, gain_attn, wq, bias, keys, values, wo, gain_ffn, wg, wu, wd,
    normed, value_t, wd_t, hid_t, wo_e, work, outs, lsplit, stage2, stage6,
    own1, own4, held1, line3, held4, buf1, buf3, buf4, plane2, plane6, rel2, rel6, held2, held6,
    gu, gstage, gbuf, act, res,
    in_sem, zsend, zrecv, psend, precv, rrecv, asem,
):
    s = lax.axis_index("seq")
    m = lax.axis_index("mp")
    z, x, yh = lax.rem(s, LINE), lax.rem(s // LINE, 4), s // (4 * LINE)
    yl, c = m // 2, lax.rem(m, 2)
    line = s - z
    here = s // LINE
    xb = lax.rem(x, 2)
    own_j = LINE * xb + z
    mine = x // 2 == c
    same_y = yl == yh

    bar = pltpu.get_barrier_semaphore()

    def greet(p, q):
        pl.semaphore_signal(bar, inc=1, device_id=(p, q), device_id_type=MESH)

    for d in (4, 3, 5, 2, 6, 1, 7, 0):
        for u, v in ((1, 0), (1, 1), (0, 1), (0, 0)):
            if d or u or v:
                greet(32 * lax.rem(yh + u, 2) + LINE * x + lax.rem(z + d, LINE), 2 * lax.rem(yl + v, 2) + c)
    for i in (2, 1, 3):
        greet(32 * (1 - yh) + LINE * lax.rem(x + i, 4) + z, m)
    for i in (6, 2, 5, 7, 1, 3, 4):
        greet(32 * yh + LINE * lax.rem(x + i % 4, 4) + z, 2 * yl + lax.rem(c + i // 4, 2))
    greet(s, 2 * (1 - yl) + 1 - c)

    pairs = (
        (tokens_h, tokens), (gain_attn_h, gain_attn), (wq_h, wq), (bias_h, bias),
        (keys_h.at[m], keys), (values_h.at[m], values), (wo_h, wo), (gain_ffn_h, gain_ffn),
        (wg_h, wg), (wu_h, wu), (wd_h, wd.at[pl.ds(0, HID)]),
    )
    loads = [pltpu.make_async_copy(a, b, in_sem.at[i]) for i, (a, b) in enumerate(pairs)]
    for load in loads:
        load.start()

    loads[0].wait()
    loads[1].wait()
    normed[pl.ds(TOK, TOK), :] = jnp.zeros((TOK, D), BF)
    gain_row = jnp.concatenate([gain_attn[i : i + 1, :] for i in range(D // 128)], axis=1)

    def norm_rows(i, c):
        at = pl.multiple_of(i * 16, 16)
        x = tokens[pl.ds(at, 16), :].astype(F32)
        mean_sq = jnp.sum(x * x, axis=1, keepdims=True) * (1.0 / D)
        normed[pl.ds(at, 16), :] = (x * lax.rsqrt(mean_sq + EPS) * gain_row).astype(BF)
        return c

    lax.fori_loop(0, TOK // 16, norm_rows, 0)
    loads[2].wait()
    loads[3].wait()
    q_t = dot(wq[...], normed[...], ((1,), (1,))) + column_of(bias[...])
    low32 = low_lanes(PK)

    def packed(x):
        hi = jnp.concatenate([x[PK:COL], jnp.zeros((8, 128), F32)], axis=0)
        return jnp.where(low32, x[0:PK], swap(hi))

    def remote(src, dst, send_sem, recv_sem, p, q):
        pltpu.make_async_remote_copy(
            src_ref=src, dst_ref=dst, send_sem=send_sem, recv_sem=recv_sem, device_id=(p, q), device_id_type=MESH
        ).start()

    def copy(src, dst, send_sem, recv_sem, p, q, local):
        @pl.when(local)
        def _():
            pltpu.make_async_copy(src, dst, recv_sem).start()

        @pl.when(jnp.logical_not(local))
        def _():
            remote(src, dst, send_sem, recv_sem, p, q)

    def arrived(buf, sem):
        pltpu.make_async_copy(buf, buf, sem).wait()

    def near_first(i):
        return lax.rem(jnp.where(lax.rem(i, 2) == 1, (i + 1) // 2, LINE - i // 2), LINE)

    def far_first(i):
        return lax.rem(LINE + LINE // 2 + jnp.where(lax.rem(i, 2) == 1, -((i + 1) // 2), i // 2), LINE)

    def spread_yz(own, held, k):
        for d in (4, 3, 5, 2, 6, 1, 7, 0):
            for u in range(2):
                to = (32 * u + LINE * x + lax.rem(z + d, LINE), 2 * yh + c)
                sems = (zsend.at[k], zrecv.at[k, yl, (LINE - d) % LINE])
                slot = held.at[yl, z]
                if d:
                    remote(own, slot, *sems, *to)
                else:
                    copy(own, slot, *sems, *to, jnp.logical_and(yh == u, same_y))

    def spread_x(held, buf, k):
        for t in range(2):

            def step(i, carry, t=t):
                e = near_first(i)
                at = lax.rem(z + e, LINE)
                arrived(held.at[t, at], zrecv.at[k, t, e])
                for o in (2, 1, 3, 0):
                    to = (32 * yh + LINE * lax.rem(x + o, 4) + z, 2 * yl + x // 2)
                    args = (held.at[t, at], buf.at[t, 2 * xb + c, at], psend.at[k], precv.at[k, t], *to)
                    if o:
                        remote(*args)
                    else:
                        copy(*args, mine)
                return carry

            lax.fori_loop(0, LINE, step, 0)

    def along_line(held, k):
        for d in (4, 3, 5, 2, 6, 1, 7):
            remote(held.at[z], held.at[z], zsend.at[k], zrecv.at[k, 0, LINE - d], line + lax.rem(z + d, LINE), m)

    def on_to_plane(held, buf, k):
        def step(i, carry):
            e = near_first(i)
            at = lax.rem(z + e, LINE)

            @pl.when(i > 0)
            def _():
                arrived(held.at[at], zrecv.at[k, 0, e])

            for d in range(1, 8):
                p = LINE * lax.rem(here + d, 8) + z
                remote(held.at[at], buf.at[here, at], psend.at[k], precv.at[k, 0], p, m)
            pltpu.make_async_copy(held.at[at], buf.at[here, at], precv.at[k, 0]).start()
            return carry

        lax.fori_loop(0, LINE, step, 0)

    own1[...] = packed(q_t).astype(BF)

    loads[5].wait()
    value_t[...] = values[...].T
    first = lax.broadcasted_iota(jnp.int32, (COL, D), 1) - lax.broadcasted_iota(jnp.int32, (COL, D), 0)
    pick = jnp.where(first == s * COL, 1.0, 0.0).astype(BF)
    normed[pl.ds(0, TOK), :] = tokens[...]
    hid_t[...] = dot(pick, normed[...], ((1,), (1,)))
    loads[10].wait()
    wd[pl.ds(HID, HIDP - HID), :] = jnp.zeros((HIDP - HID, FEAT), BF)
    wd_t[...] = wd[...].T
    outs[pl.ds(FEAT, 8), :] = jnp.zeros((8, ALL), F32)
    gu[:, pl.ds(HID, HIDP - HID), :] = jnp.zeros((2, HIDP - HID, ALL), F32)
    wide = PEER * PK
    c_at = lax.broadcasted_iota(jnp.int32, (FEAT, wide), 1)
    r_at = lax.broadcasted_iota(jnp.int32, (FEAT, wide), 0) - COL * (c_at // PK)
    c_at = lax.rem(c_at, PK)
    pick_lo = jnp.where(r_at == c_at, 1.0, 0.0).astype(BF)
    pick_hi = jnp.where(jnp.logical_and(r_at == c_at + PK, c_at < COL - PK), 1.0, 0.0).astype(BF)
    wo_e[...] = jnp.zeros((128, SEQ * PK), BF)
    loads[6].wait()
    for i in range(MP):
        part = wo[:, pl.ds(i * FEAT, FEAT)]
        wo_e[pl.ds(0, COL), pl.ds(i * wide, wide)] = dot(part, pick_lo).astype(BF)
        wo_e[pl.ds(64, COL), pl.ds(i * wide, wide)] = dot(part, pick_hi).astype(BF)
    for i in (4, 7, 8, 9):
        loads[i].wait()

    pl.semaphore_wait(bar, 42)
    spread_yz(own1, held1, 0)
    spread_x(held1, buf1, 0)

    def unpack_chunks(buf, t, squares):
        tile = pl.ds(128 * t, 128)

        def one(j, total):
            a = buf[t, 2 * (j // LINE), lax.rem(j, LINE)].astype(F32)
            b = buf[t, 2 * (j // LINE) + 1, lax.rem(j, LINE)].astype(F32)
            lo = jnp.where(low32, a, swap(b))
            hi = jnp.where(low32, swap(a), b)
            at = pl.multiple_of(j * COL, 8)
            work[pl.ds(at, PK), tile] = lo
            work[pl.ds(pl.multiple_of(at + PK, 8), COL - PK), tile] = hi[0 : COL - PK]
            return total + hi[COL - PK : PK] if squares else total

        return lax.fori_loop(0, PEER, one, jnp.zeros((8, 128), F32), unroll=4)

    low8 = low_lanes(8)

    def collect_x(stage, plane, k, t, halves, stats):
        tile = pl.ds(128 * t, 128)

        def step(i, carry):
            e = far_first(i)
            to_z = lax.rem(z + e, LINE)
            for half in halves:
                j = half * LINE + to_z
                r = outs[pl.ds(pl.multiple_of(j * COL, 8), 2 * PK), tile]
                lo, hi = r[0:PK], r[PK : 2 * PK]
                a = jnp.where(low32, lo, swap(hi))
                b = jnp.where(low32, swap(lo), hi)
                if stats:
                    h0, h1 = (j * COL) // HEAD, (j * COL + COL - 1) // HEAD
                    both = jnp.where(row_ids(8) < 3, lsplit[h0, :, tile], lsplit[h1, :, tile])
                    a = jnp.concatenate([a[0:24], jnp.where(low8, a[24:PK], swap(both))], axis=0)
                    b = jnp.concatenate([b[0:24], jnp.where(low8, b[24:PK], both)], axis=0)
                stage[t, to_z, 2 * half] = a.astype(BF)
                stage[t, to_z, 2 * half + 1] = b.astype(BF)
            for g in [2 * half + i for half in halves for i in range(2)]:
                to = (32 * yh + LINE * (2 * c + g // 2) + z, 2 * yl + g % 2)
                local = jnp.logical_and(2 * c + g // 2 == x, g % 2 == c)
                copy(stage.at[t, to_z, g], plane.at[t, to_z, x], psend.at[k], rrecv.at[k, t, e], *to, local)
            return carry

        lax.fori_loop(0, LINE, step, 0)

    def collect_yz(plane, rel, held, k, join):
        for t in range(2):

            def step(i, carry, t=t):
                e = far_first(i)
                to_z = lax.rem(z + e, LINE)
                arrived(plane.at[t, to_z], rrecv.at[k, t, e])
                rel[t, to_z] = join(plane[t, to_z].astype(F32), to_z).astype(BF)
                local = jnp.logical_and(jnp.logical_and(same_y, e == 0), yl == t)
                to = (32 * yl + LINE * x + to_z, 2 * t + c)
                copy(rel.at[t, to_z], held.at[2 * z + yh], zsend.at[k], zrecv.at[k, 0, 0], *to, local)
                return carry

            lax.fori_loop(0, LINE, step, 0)
        arrived(held, zrecv.at[k, 0, 0])

    scale = HEAD ** (-0.5) * LOG2E

    def attend(t, h, n):
        tile = pl.ds(128 * t, 128)
        rows = [pl.ds(pl.multiple_of((h + i) * HEAD, HEAD), HEAD) for i in range(n)]
        queries = jnp.concatenate([work[r, tile].astype(BF) for r in rows], axis=1)
        scores = dot(keys[...], queries) * scale
        top = jnp.max(scores, axis=0, keepdims=True)
        probs = jnp.exp2(scores - top)
        total = jnp.sum(probs, axis=0, keepdims=True)
        value = dot(value_t[...], probs.astype(BF)) * (1.0 / total)
        level = top + jnp.log(total) * LOG2E
        parts = three_rows(level, 8) + three_rows(level, 8, 3)
        for i in range(n):
            outs[rows[i], tile] = value[:, 128 * i : 128 * (i + 1)]
            lsplit[h + i, :, tile] = parts[:, 128 * i : 128 * (i + 1)]

    for t in range(2):
        arrived(buf1.at[t], precv.at[0, t])
        unpack_chunks(buf1, t, False)

        def two_heads(i, carry, t=t):
            attend(t, 2 * i, 2)
            return carry

        lax.fori_loop(0, 2, two_heads, 0)
        collect_x(stage2, plane2, 1, t, (0,), True)
        attend(t, 4, 2)
        attend(t, 6, 1)
        collect_x(stage2, plane2, 1, t, (1,), True)

    def join2(chunks, to_z):
        value, levels = merge(chunks, LINE * xb + to_z)
        rows = three_rows(levels[0], 8) + three_rows(levels[1], 8, 3)
        return jnp.concatenate([value[0:24], jnp.where(low8, value[24:PK], rows)], axis=0)

    collect_yz(plane2, rel2, held2, 1, join2)
    merged = merge(held2[...].astype(F32), own_j)[0].astype(BF)
    line3[z] = merged

    along_line(line3, 2)
    on_to_plane(line3, buf3, 2)

    def unpacked(x, out):
        out[pl.ds(0, PK), :] = x[:, 0:64]
        out[pl.ds(PK, COL - PK), :] = swap(x)[0 : COL - PK, 0:64]

    unpacked(merged.astype(F32), att_out)
    res_hid = packed(hid_t[...])
    gain_col = jnp.broadcast_to(column_of(gain_ffn[...]), (COL, 128))
    gain_pk = packed(gain_col)
    arrived(buf3, precv.at[2, 0])
    both = dot(wo_e[...], buf3[...].reshape(SEQ * PK, 128))
    residual = res_hid + packed(both[0:COL] + swap(both[64 : 64 + COL]))
    res[...] = residual

    real = jnp.logical_or(low32, row_ids(PK) < COL - PK)
    squares = jnp.sum(jnp.where(real, residual * residual, 0.0), axis=0, keepdims=True)
    squares = squares + swap(squares)
    scaled = residual * gain_pk
    own4[...] = jnp.where(real, scaled, three_rows(squares, PK, 24)).astype(BF)
    spread_yz(own4, held4, 3)
    spread_x(held4, buf4, 3)

    def rows_of(core):
        return pl.ds(pl.multiple_of(core * SHARE, 16), SHARE)

    def put_sums(ref, gate, up, sq):
        ref[pl.ds(0, SHARE)] = gate.astype(BF)
        ref[pl.ds(SHARE, SHARE)] = up.astype(BF)
        ref[pl.ds(2 * SHARE, 16)] = three_rows(sq, 16).astype(BF)

    def add_sums(ref, gate, up, sq):
        gate = gate + ref[pl.ds(0, SHARE)].astype(F32)
        up = up + ref[pl.ds(SHARE, SHARE)].astype(F32)
        return gate, up, sq + jnp.sum(ref[pl.ds(2 * SHARE, 16)].astype(F32), axis=0, keepdims=True)

    sqs = []
    for t in range(2):
        tile = pl.ds(128 * t, 128)
        arrived(buf4.at[t], precv.at[3, t])
        sq = jnp.sum(unpack_chunks(buf4, t, True), axis=0, keepdims=True)
        features = work[pl.ds(0, FEAT), tile].astype(BF)
        gu[0, pl.ds(0, HID), tile] = dot(wg[...], features)
        gu[1, pl.ds(0, HID), tile] = dot(wu[...], features)
        put_sums(gstage.at[t, 0], gu[0, rows_of(1 - c), tile], gu[1, rows_of(1 - c), tile], sq)
        remote(gstage.at[t, 0], gbuf.at[t, 0], asem.at[0, t, 0], asem.at[1, t, 0], s, 2 * yl + 1 - c)
        sqs.append(sq)
    sums = []
    for t in range(2):
        tile = pl.ds(128 * t, 128)
        arrived(gbuf.at[t, 0], asem.at[1, t, 0])
        gate, up, sq = add_sums(gbuf.at[t, 0], gu[0, rows_of(c), tile], gu[1, rows_of(c), tile], sqs[t])
        put_sums(gstage.at[t, 1], gate, up, sq)
        remote(gstage.at[t, 1], gbuf.at[t, 1], asem.at[0, t, 1], asem.at[1, t, 1], s, 2 * (1 - yl) + c)
        sums.append((gate, up, sq))
    for t in range(2):
        arrived(gbuf.at[t, 1], asem.at[1, t, 1])
        gate, up, sq = add_sums(gbuf.at[t, 1], *sums[t])
        factor = lax.rsqrt(sq * (1.0 / D) + EPS)
        gate = gate * factor
        up = up * factor
        act[t, rows_of(c)] = (gate / (1.0 + jnp.exp(-gate)) * up).astype(BF)
        part = act.at[t, rows_of(c)]
        remote(part, part, asem.at[0, t, 2], asem.at[1, t, 2], s, 2 * yl + 1 - c)

    for t in range(2):
        arrived(act.at[t, rows_of(1 - c)], asem.at[1, t, 2])
        outs[pl.ds(0, FEAT), pl.ds(128 * t, 128)] = dot(wd_t[...], act[t])
        collect_x(stage6, plane6, 4, t, (0, 1), False)
    collect_yz(plane6, rel6, held6, 4, lambda chunks, to_z: jnp.sum(chunks, axis=0))
    unpacked(res[...] + jnp.sum(held6[...].astype(F32), axis=0), lay_out)

    fifteen, most = held2.at[pl.ds(0, 15)], buf3.at[pl.ds(0, 6)]
    for k in (0, 1, 3, 4):
        for own, part, whole, sem in ((same_y, fifteen, held2, zsend.at[k]), (mine, most, buf3, psend.at[k])):

            @pl.when(own)
            def _(part=part, sem=sem):
                arrived(part, sem)

            @pl.when(jnp.logical_not(own))
            def _(whole=whole, sem=sem):
                arrived(whole, sem)

    arrived(line3.at[pl.ds(0, 7)], zsend.at[2])
    arrived(buf3.at[pl.ds(0, 7)], psend.at[2])
    for t in range(2):
        arrived(gstage.at[t, 0], asem.at[0, t, 0])
        arrived(gstage.at[t, 1], asem.at[0, t, 1])
        arrived(act.at[t, rows_of(c)], asem.at[0, t, 2])


def body(tokens, gain_attn, w_query, query_bias, cache_keys, cache_values, w_out, gain_ffn, w_gate, w_up, w_down):
    v = pltpu.VMEM
    one, eight, pairs, halves = (PK, 128), (LINE, PK, 128), (2 * LINE, PK, 128), (2, LINE, PK, 128)
    chunks, users, owners = (8, LINE, PK, 128), (2, 4, LINE, PK, 128), (2, LINE, 4, PK, 128)
    sem = pltpu.SemaphoreType.DMA
    scratch = [
        v((TOK, D), BF), v((D // 128, 128), F32), v((COL, D), BF), v((1, COL), F32), v((CTX, HEAD), BF),
        v((CTX, HEAD), BF), v((COL, D), BF), v((1, COL), F32), v((HID, FEAT), BF), v((HID, FEAT), BF),
        v((HIDP, FEAT), BF),
        v((2 * TOK, D), BF),
        v((HEAD, CTX), BF),
        v((FEAT, HIDP), BF),
        v((COL, 128), F32),
        v((128, SEQ * PK), BF),
        v((FEAT, ALL), F32),
        v((FEAT + 8, ALL), F32),
        v((8, 8, ALL), F32),
        v(owners, BF), v(owners, BF),
        v(one, BF), v(one, BF), v(halves, BF), v(eight, BF), v(halves, BF),
        v(users, BF), v(chunks, BF), v(users, BF),
        v(owners, BF), v(owners, BF),
        v(halves, BF), v(halves, BF), v(pairs, BF), v(pairs, BF),
        v((2, HIDP, ALL), F32),
        v((2, 2, 2 * SHARE + 16, 128), BF), v((2, 2, 2 * SHARE + 16, 128), BF),
        v((2, HIDP, 128), BF),
        v((PK, 128), F32),
        sem((11,)), sem((5,)), sem((5, 2, LINE)), sem((5,)), sem((5, 2)), sem((5, 2, LINE)), sem((2, 2, 3)),
    ]
    any_space = pl.BlockSpec(memory_space=pl.ANY)
    attended, layer = pl.pallas_call(
        kernel,
        out_shape=(jax.ShapeDtypeStruct((COL, TOK), F32), jax.ShapeDtypeStruct((COL, TOK), F32)),
        in_specs=[any_space] * 11,
        out_specs=(pl.BlockSpec(memory_space=pltpu.VMEM), pl.BlockSpec(memory_space=pltpu.VMEM)),
        scratch_shapes=scratch,
        compiler_params=pltpu.CompilerParams(
            collective_id=0, has_side_effects=True, vmem_limit_bytes=66700000
        ),
        name="layer",
    )(
        tokens, gain_attn.reshape(D // 128, 128), w_query.T, query_bias.reshape(1, COL), cache_keys, cache_values,
        w_out.T, gain_ffn.reshape(1, COL), w_gate.T, w_up.T, w_down,
    )
    return attended.T.astype(BF), layer.T.astype(BF)


def solution(mesh):
    placed = (
        P("mp", None), P(), P(None, "seq"), P("seq"), P(None, "seq", None), P(None, "seq", None),
        P(None, "seq"), P("seq"), P("mp", "seq"), P("mp", "seq"), P("seq", "mp"),
    )
    return jax.shard_map(
        body, mesh=mesh, in_specs=placed, out_specs=(P("mp", "seq"), P("mp", "seq")), check_vma=False
    )
```

```python
import functools
import math

import jax
import jax.numpy as jnp
from jax import lax
from jax.experimental import pallas as pl
from jax.experimental.pallas import tpu as pltpu
from jax.sharding import PartitionSpec as P

D = 3584
HEAD = 128
GROUP = 7
KV = 4
CTX = 1024
SEQ = 64
MP = 4
TOK = 64
ALL = TOK * MP
COL = 56
FEAT = D // MP
PEER = FEAT // COL
HID = 296
SHARE = 160
HIDP = 2 * SHARE
PK = 32
LINE = 8
EPS = 1e-06
MESH = pl.DeviceIdType.MESH
BF = jnp.bfloat16
F32 = jnp.float32
LOG2E = 1.0 / math.log(2.0)


def dot(a, b, dims=((1,), (0,))):
    return lax.dot_general(a, b, (dims, ((), ())), preferred_element_type=F32)


def low_lanes(rows):
    return lax.broadcasted_iota(jnp.int32, (rows, 128), 1) < 64


def row_ids(rows):
    return lax.broadcasted_iota(jnp.int32, (rows, 128), 0)


def swap(x):
    return pltpu.roll(x, 64, axis=1)


def column_of(row):
    n = row.shape[1]
    same = lax.broadcasted_iota(jnp.int32, (n, n), 0) == lax.broadcasted_iota(jnp.int32, (n, n), 1)
    return jnp.sum(jnp.where(same, jnp.broadcast_to(row, (n, n)), 0.0), axis=1, keepdims=True)


def split3(x):
    first = x.astype(BF).astype(F32)
    rest = x - first
    second = rest.astype(BF).astype(F32)
    return first, second, rest - second


def three_rows(x, rows, base=0):
    first, second, third = split3(x)
    at = lax.broadcasted_iota(jnp.int32, (rows, x.shape[1]), 0) - base
    return jnp.where(at == 0, first, jnp.where(at == 1, second, jnp.where(at == 2, third, 0.0)))


def merge(chunks, j):
    at = row_ids(8)
    high = jnp.logical_not(low_lanes(chunks.shape[0]))
    sides = ([], [])
    for i in range(chunks.shape[0]):
        part = chunks[i, 24:PK]
        sides[0].append(jnp.sum(jnp.where(at < 3, part, 0.0), axis=0, keepdims=True))
        sides[1].append(jnp.sum(jnp.where(jnp.logical_and(at >= 3, at < 6), part, 0.0), axis=0, keepdims=True))
    weights, levels = [], []
    for rows in sides:
        level = jnp.concatenate(rows, axis=0)
        level = jnp.where(high, level, swap(level))
        top = jnp.max(level, axis=0, keepdims=True)
        weight = jnp.exp2(level - top)
        total = jnp.sum(weight, axis=0, keepdims=True)
        weights.append(weight / total)
        levels.append(top + jnp.log(total) * LOG2E)
    edge = HEAD * ((j * COL) // HEAD + 1) - j * COL
    first_head = row_ids(PK) + jnp.where(low_lanes(PK), 0, PK) < edge
    acc = jnp.zeros((PK, 128), F32)
    for i in range(chunks.shape[0]):
        acc += chunks[i] * jnp.where(first_head, weights[0][i : i + 1], weights[1][i : i + 1])
    return acc, levels


def kernel(
    tokens_h, gain_attn_h, wq_h, bias_h, keys_h, values_h, wo_h, gain_ffn_h, wg_h, wu_h, wd_h,
    att_out, lay_out,
    tokens, gain_attn, wq, bias, keys, values, wo, gain_ffn, wg, wu, wd,
    normed, value_t, wd_t, hid_t, wo_e, work, outs, lsplit, stage2, stage6,
    own1, own3, own4, held1, line3, held4, buf1, buf3, buf4, plane2, plane6, rel2, rel6, held2, held6,
    gu, gstage, gbuf, act, res, many,
    in_sem, zsend, zrecv, psend, precv, rrecv, asem,
):
    s = lax.axis_index("seq")
    m = lax.axis_index("mp")
    z, x, yh = lax.rem(s, LINE), lax.rem(s // LINE, 4), s // (4 * LINE)
    yl, c = m // 2, lax.rem(m, 2)
    line = s - z
    here = s // LINE
    xb = lax.rem(x, 2)
    own_j = LINE * xb + z
    mine = x // 2 == c
    same_y = yl == yh
    relay = c == 1

    bar = pltpu.get_barrier_semaphore()

    def greet(p, q):
        pl.semaphore_signal(bar, inc=1, device_id=(p, q), device_id_type=MESH)

    for d in (4, 3, 5, 2, 6, 1, 7, 0):
        for u, v in ((1, 0), (1, 1), (0, 1), (0, 0)):
            for w in range(2):
                if d or u or v or w:
                    p = 32 * lax.rem(yh + u, 2) + LINE * x + lax.rem(z + d, LINE)
                    greet(p, 2 * lax.rem(yl + v, 2) + lax.rem(c + w, 2))
    for i in (2, 1, 3):
        for u in (1, 0):
            for w in range(2):
                p = 32 * lax.rem(yh + u, 2) + LINE * lax.rem(x + i, 4) + z
                greet(p, 2 * yl + lax.rem(c + w, 2))

    pairs = (
        (tokens_h, tokens), (gain_attn_h, gain_attn), (wq_h, wq), (bias_h, bias),
        (keys_h.at[m], keys), (values_h.at[m], values), (wo_h, wo), (gain_ffn_h, gain_ffn),
        (wg_h, wg), (wu_h, wu), (wd_h, wd.at[pl.ds(0, HID)]),
    )
    loads = [pltpu.make_async_copy(a, b, in_sem.at[i]) for i, (a, b) in enumerate(pairs)]
    for load in loads:
        load.start()

    loads[0].wait()
    loads[1].wait()
    normed[pl.ds(TOK, TOK), :] = jnp.zeros((TOK, D), BF)
    gain_row = jnp.concatenate([gain_attn[i : i + 1, :] for i in range(D // 128)], axis=1)

    def norm_rows(i, c):
        at = pl.multiple_of(i * 16, 16)
        x = tokens[pl.ds(at, 16), :].astype(F32)
        mean_sq = jnp.sum(x * x, axis=1, keepdims=True) * (1.0 / D)
        normed[pl.ds(at, 16), :] = (x * lax.rsqrt(mean_sq + EPS) * gain_row).astype(BF)
        return c

    lax.fori_loop(0, TOK // 16, norm_rows, 0)
    loads[2].wait()
    loads[3].wait()
    q_t = dot(wq[...], normed[...], ((1,), (1,))) + column_of(bias[...])
    low32 = low_lanes(PK)

    def packed(x):
        hi = jnp.concatenate([x[PK:COL], jnp.zeros((8, 128), F32)], axis=0)
        return jnp.where(low32, x[0:PK], swap(hi))

    def remote(src, dst, send_sem, recv_sem, p, q):
        pltpu.make_async_remote_copy(
            src_ref=src, dst_ref=dst, send_sem=send_sem, recv_sem=recv_sem, device_id=(p, q), device_id_type=MESH
        ).start()

    def copy(src, dst, send_sem, recv_sem, p, q, local):
        @pl.when(local)
        def _():
            pltpu.make_async_copy(src, dst, recv_sem).start()

        @pl.when(jnp.logical_not(local))
        def _():
            remote(src, dst, send_sem, recv_sem, p, q)

    def arrived(buf, sem):
        pltpu.make_async_copy(buf, buf, sem).wait()

    def near_first(i):
        return lax.rem(jnp.where(lax.rem(i, 2) == 1, (i + 1) // 2, LINE - i // 2), LINE)

    def far_first(i):
        return lax.rem(LINE + LINE // 2 + jnp.where(lax.rem(i, 2) == 1, -((i + 1) // 2), i // 2), LINE)

    def spread_yz(own, held, k):
        for d in (4, 3, 5, 2, 6, 1, 7, 0):
            for u in range(2):
                to = (32 * u + LINE * x + lax.rem(z + d, LINE), 2 * yh + 1)
                sems = (zsend.at[k], zrecv.at[k, yl, (LINE - d) % LINE])
                slot = held.at[yl, z, c]
                if d:
                    remote(own, slot, *sems, *to)
                else:
                    copy(own, slot, *sems, *to, jnp.logical_and(jnp.logical_and(yh == u, same_y), relay))

    def spread_x(held, buf, k):
        def pass_on():
            for t in range(2):

                def step(i, carry, t=t):
                    e = near_first(i)
                    at = lax.rem(z + e, LINE)
                    arrived(held.at[t, at], zrecv.at[k, t, e])
                    for o in (2, 1, 3, 0):
                        to = (32 * yh + LINE * lax.rem(x + o, 4) + z, 2 * yl + x // 2)
                        args = (held.at[t, at], buf.at[t, xb, at], psend.at[k], precv.at[k, t], *to)
                        if o:
                            remote(*args)
                        else:
                            copy(*args, x // 2 == 1)
                    return carry

                lax.fori_loop(0, LINE, step, 0)

        pl.when(relay)(pass_on)

    def along_line(own, held, k):
        for d in (4, 3, 5, 2, 6, 1, 7, 0):
            to = (line + lax.rem(z + d, LINE), 2 * yl + 1)
            args = (own, held.at[z, c], zsend.at[k], zrecv.at[k, 0, (LINE - d) % LINE], *to)
            if d:
                remote(*args)
            else:
                copy(*args, relay)

    def on_to_plane(held, buf, k):
        def pass_on():
            def step(i, carry):
                e = near_first(i)
                at = lax.rem(z + e, LINE)
                arrived(held.at[at], zrecv.at[k, 0, e])
                for w in range(2):
                    for d in (6, 2, 5, 7, 1, 3, 4):
                        p = LINE * lax.rem(here + d, 8) + z
                        remote(held.at[at, w], buf.at[here, at], psend.at[k], precv.at[k, 0], p, 2 * yl + w)
                remote(held.at[at, 0], buf.at[here, at], psend.at[k], precv.at[k, 0], s, 2 * yl)
                pltpu.make_async_copy(held.at[at, 1], buf.at[here, at], precv.at[k, 0]).start()
                return carry

            lax.fori_loop(0, LINE, step, 0)

        pl.when(relay)(pass_on)

    own1[...] = packed(q_t).astype(BF)

    loads[5].wait()
    value_t[...] = values[...].T
    first = lax.broadcasted_iota(jnp.int32, (COL, D), 1) - lax.broadcasted_iota(jnp.int32, (COL, D), 0)
    pick = jnp.where(first == s * COL, 1.0, 0.0).astype(BF)
    normed[pl.ds(0, TOK), :] = tokens[...]
    hid_t[...] = dot(pick, normed[...], ((1,), (1,)))
    loads[10].wait()
    wd[pl.ds(HID, HIDP - HID), :] = jnp.zeros((HIDP - HID, FEAT), BF)
    wd_t[...] = wd[...].T
    outs[pl.ds(FEAT, 8), :] = jnp.zeros((8, ALL), F32)
    gu[:, pl.ds(HID, HIDP - HID), :] = jnp.zeros((2, HIDP - HID, ALL), F32)
    wide = PEER * PK
    c_at = lax.broadcasted_iota(jnp.int32, (FEAT, wide), 1)
    r_at = lax.broadcasted_iota(jnp.int32, (FEAT, wide), 0) - COL * (c_at // PK)
    c_at = lax.rem(c_at, PK)
    pick_lo = jnp.where(r_at == c_at, 1.0, 0.0).astype(BF)
    pick_hi = jnp.where(jnp.logical_and(r_at == c_at + PK, c_at < COL - PK), 1.0, 0.0).astype(BF)
    wo_e[...] = jnp.zeros((128, SEQ * PK), BF)
    loads[6].wait()
    for i in range(MP):
        part = wo[:, pl.ds(i * FEAT, FEAT)]
        wo_e[pl.ds(0, COL), pl.ds(i * wide, wide)] = dot(part, pick_lo).astype(BF)
        wo_e[pl.ds(64, COL), pl.ds(i * wide, wide)] = dot(part, pick_hi).astype(BF)
    for i in (4, 7, 8, 9):
        loads[i].wait()

    pl.semaphore_wait(bar, 75)
    spread_yz(own1, held1, 0)
    spread_x(held1, buf1, 0)

    def unpack_chunks(buf, t, squares):
        tile = pl.ds(128 * t, 128)

        def one(j, total):
            a = buf[t, j // LINE, lax.rem(j, LINE), 0].astype(F32)
            b = buf[t, j // LINE, lax.rem(j, LINE), 1].astype(F32)
            lo = jnp.where(low32, a, swap(b))
            hi = jnp.where(low32, swap(a), b)
            at = pl.multiple_of(j * COL, 8)
            work[pl.ds(at, PK), tile] = lo
            work[pl.ds(pl.multiple_of(at + PK, 8), COL - PK), tile] = hi[0 : COL - PK]
            return total + hi[COL - PK : PK] if squares else total

        return lax.fori_loop(0, PEER, one, jnp.zeros((8, 128), F32), unroll=4)

    low8 = low_lanes(8)

    def collect_x(stage, plane, k, t, halves, stats):
        tile = pl.ds(128 * t, 128)

        def step(i, carry):
            e = far_first(i)
            to_z = lax.rem(z + e, LINE)
            for half in halves:
                j = half * LINE + to_z
                r = outs[pl.ds(pl.multiple_of(j * COL, 8), 2 * PK), tile]
                lo, hi = r[0:PK], r[PK : 2 * PK]
                a = jnp.where(low32, lo, swap(hi))
                b = jnp.where(low32, swap(lo), hi)
                if stats:
                    h0, h1 = (j * COL) // HEAD, (j * COL + COL - 1) // HEAD
                    both = jnp.where(row_ids(8) < 3, lsplit[h0, :, tile], lsplit[h1, :, tile])
                    a = jnp.concatenate([a[0:24], jnp.where(low8, a[24:PK], swap(both))], axis=0)
                    b = jnp.concatenate([b[0:24], jnp.where(low8, b[24:PK], both)], axis=0)
                stage[t, to_z, half, 0] = a.astype(BF)
                stage[t, to_z, half, 1] = b.astype(BF)
            for half in halves:
                to = (32 * yh + LINE * (2 * c + half) + z, 2 * yl + 1)
                local = jnp.logical_and(2 * c + half == x, relay)
                copy(stage.at[t, to_z, half], plane.at[t, to_z, x], psend.at[k], rrecv.at[k, t, e], *to, local)
            return carry

        lax.fori_loop(0, LINE, step, 0)

    def collect_yz(plane, rel, held, k, join):
        def pass_on():
            for t in range(2):

                def step(i, carry, t=t):
                    e = far_first(i)
                    to_z = lax.rem(z + e, LINE)
                    arrived(plane.at[t, to_z], rrecv.at[k, t, e])
                    for w in range(2):
                        rel[t, to_z, w] = join(plane[t, to_z, :, w].astype(F32), to_z).astype(BF)
                        args = (rel.at[t, to_z, w], held.at[2 * z + yh], zsend.at[k], zrecv.at[k, 0, 0])
                        to = (32 * yl + LINE * x + to_z, 2 * t + w)
                        if w:
                            copy(*args, *to, jnp.logical_and(jnp.logical_and(same_y, e == 0), yl == t))
                        else:
                            remote(*args, *to)
                    return carry

                lax.fori_loop(0, LINE, step, 0)

        pl.when(relay)(pass_on)
        arrived(held, zrecv.at[k, 0, 0])

    scale = HEAD ** (-0.5) * LOG2E

    def attend(t, h, n):
        tile = pl.ds(128 * t, 128)
        rows = [pl.ds(pl.multiple_of((h + i) * HEAD, HEAD), HEAD) for i in range(n)]
        queries = jnp.concatenate([work[r, tile].astype(BF) for r in rows], axis=1)
        scores = dot(keys[...], queries) * scale
        top = jnp.max(scores, axis=0, keepdims=True)
        probs = jnp.exp2(scores - top)
        total = jnp.sum(probs, axis=0, keepdims=True)
        value = dot(value_t[...], probs.astype(BF)) * (1.0 / total)
        level = top + jnp.log(total) * LOG2E
        parts = three_rows(level, 8) + three_rows(level, 8, 3)
        for i in range(n):
            outs[rows[i], tile] = value[:, 128 * i : 128 * (i + 1)]
            lsplit[h + i, :, tile] = parts[:, 128 * i : 128 * (i + 1)]

    for t in range(2):
        arrived(buf1.at[t], precv.at[0, t])
        unpack_chunks(buf1, t, False)

        def two_heads(i, carry, t=t):
            attend(t, 2 * i, 2)
            return carry

        lax.fori_loop(0, GROUP // 2, two_heads, 0)
        attend(t, GROUP - 1, 1)
        collect_x(stage2, plane2, 1, t, (0, 1), True)

    def join2(chunks, to_z):
        value, levels = merge(chunks, LINE * xb + to_z)
        rows = three_rows(levels[0], 8) + three_rows(levels[1], 8, 3)
        return jnp.concatenate([value[0:24], jnp.where(low8, value[24:PK], rows)], axis=0)

    collect_yz(plane2, rel2, held2, 1, join2)
    merged = merge(held2[...].astype(F32), own_j)[0].astype(BF)
    own3[...] = merged

    along_line(own3, line3, 2)
    on_to_plane(line3, buf3, 2)

    def unpacked(x, out):
        out[pl.ds(0, PK), :] = x[:, 0:64]
        out[pl.ds(PK, COL - PK), :] = swap(x)[0 : COL - PK, 0:64]

    unpacked(merged.astype(F32), att_out)
    res_hid = packed(hid_t[...])
    gain_col = jnp.broadcast_to(column_of(gain_ffn[...]), (COL, 128))
    gain_pk = packed(gain_col)
    arrived(buf3, precv.at[2, 0])
    both = dot(wo_e[...], buf3[...].reshape(SEQ * PK, 128))
    residual = res_hid + packed(both[0:COL] + swap(both[64 : 64 + COL]))
    res[...] = residual

    real = jnp.logical_or(low32, row_ids(PK) < COL - PK)
    squares = jnp.sum(jnp.where(real, residual * residual, 0.0), axis=0, keepdims=True)
    squares = squares + swap(squares)
    scaled = residual * gain_pk
    own4[...] = jnp.where(real, scaled, three_rows(squares, PK, 24)).astype(BF)
    spread_yz(own4, held4, 3)
    spread_x(held4, buf4, 3)

    def rows_of(core):
        return pl.ds(pl.multiple_of(core * SHARE, 16), SHARE)

    def put_sums(ref, gate, up, sq):
        ref[pl.ds(0, SHARE)] = gate.astype(BF)
        ref[pl.ds(SHARE, SHARE)] = up.astype(BF)
        ref[pl.ds(2 * SHARE, 16)] = three_rows(sq, 16).astype(BF)

    def add_sums(ref, gate, up, sq):
        gate = gate + ref[pl.ds(0, SHARE)].astype(F32)
        up = up + ref[pl.ds(SHARE, SHARE)].astype(F32)
        return gate, up, sq + jnp.sum(ref[pl.ds(2 * SHARE, 16)].astype(F32), axis=0, keepdims=True)

    sqs = []
    for t in range(2):
        tile = pl.ds(128 * t, 128)
        arrived(buf4.at[t], precv.at[3, t])
        sq = jnp.sum(unpack_chunks(buf4, t, True), axis=0, keepdims=True)
        features = work[pl.ds(0, FEAT), tile].astype(BF)
        gu[0, pl.ds(0, HID), tile] = dot(wg[...], features)
        gu[1, pl.ds(0, HID), tile] = dot(wu[...], features)
        put_sums(gstage.at[t, 0], gu[0, rows_of(1 - c), tile], gu[1, rows_of(1 - c), tile], sq)
        remote(gstage.at[t, 0], gbuf.at[t, 0], asem.at[0, t, 0], asem.at[1, t, 0], s, 2 * yl + 1 - c)
        sqs.append(sq)
    sums = []
    for t in range(2):
        tile = pl.ds(128 * t, 128)
        arrived(gbuf.at[t, 0], asem.at[1, t, 0])
        gate, up, sq = add_sums(gbuf.at[t, 0], gu[0, rows_of(c), tile], gu[1, rows_of(c), tile], sqs[t])
        put_sums(gstage.at[t, 1], gate, up, sq)
        remote(gstage.at[t, 1], gbuf.at[t, 1], asem.at[0, t, 1], asem.at[1, t, 1], s, 2 * (1 - yl) + c)
        sums.append((gate, up, sq))
    for t in range(2):
        arrived(gbuf.at[t, 1], asem.at[1, t, 1])
        gate, up, sq = add_sums(gbuf.at[t, 1], *sums[t])
        factor = lax.rsqrt(sq * (1.0 / D) + EPS)
        gate = gate * factor
        up = up * factor
        act[t, rows_of(c)] = (gate / (1.0 + jnp.exp(-gate)) * up).astype(BF)
        part = act.at[t, rows_of(c)]
        remote(part, part, asem.at[0, t, 2], asem.at[1, t, 2], s, 2 * yl + 1 - c)

    for t in range(2):
        arrived(act.at[t, rows_of(1 - c)], asem.at[1, t, 2])
        outs[pl.ds(0, FEAT), pl.ds(128 * t, 128)] = dot(wd_t[...], act[t])
        collect_x(stage6, plane6, 4, t, (0, 1), False)
    collect_yz(plane6, rel6, held6, 4, lambda chunks, to_z: jnp.sum(chunks, axis=0))
    unpacked(res[...] + jnp.sum(held6[...].astype(F32), axis=0), lay_out)

    def sent(cases, sem):
        for holds, n in cases:

            @pl.when(holds)
            def _(n=n):
                arrived(many.at[pl.ds(0, n)], sem)

    both_true = jnp.logical_and
    no = jnp.logical_not
    here_y = both_true(same_y, relay)
    upper = x // 2 == 1
    for k in (0, 3):
        sent(((here_y, 15), (no(here_y), 16)), zsend.at[k])
        sent(((both_true(relay, upper), 96), (both_true(relay, no(upper)), 128)), psend.at[k])
    sent(((relay, 7), (no(relay), 8)), zsend.at[2])
    sent(((relay, 120),), psend.at[2])
    for k in (1, 4):
        sent(((here_y, 31), (both_true(relay, no(same_y)), 32)), zsend.at[k])
        kept = both_true(mine, relay)
        sent(((kept, 32), (no(kept), 64)), psend.at[k])
    for t in range(2):
        arrived(gstage.at[t, 0], asem.at[0, t, 0])
        arrived(gstage.at[t, 1], asem.at[0, t, 1])
        arrived(act.at[t, rows_of(c)], asem.at[0, t, 2])


def body(tokens, gain_attn, w_query, query_bias, cache_keys, cache_values, w_out, gain_ffn, w_gate, w_up, w_down):
    v = pltpu.VMEM
    one, eight, pairs, halves = (PK, 128), (LINE, 2, PK, 128), (2 * LINE, PK, 128), (2, LINE, 2, PK, 128)
    chunks, users = (8, LINE, PK, 128), (2, 2, LINE, 2, PK, 128)
    owners, plane = (2, LINE, 2, 2, PK, 128), (2, LINE, 4, 2, PK, 128)
    sem = pltpu.SemaphoreType.DMA
    scratch = [
        v((TOK, D), BF), v((D // 128, 128), F32), v((COL, D), BF), v((1, COL), F32), v((CTX, HEAD), BF),
        v((CTX, HEAD), BF), v((COL, D), BF), v((1, COL), F32), v((HID, FEAT), BF), v((HID, FEAT), BF),
        v((HIDP, FEAT), BF),
        v((2 * TOK, D), BF),
        v((HEAD, CTX), BF),
        v((FEAT, HIDP), BF),
        v((COL, 128), F32),
        v((128, SEQ * PK), BF),
        v((FEAT, ALL), F32),
        v((FEAT + 8, ALL), F32),
        v((8, 8, ALL), F32),
        v(owners, BF), v(owners, BF),
        v(one, BF), v(one, BF), v(one, BF), v(halves, BF), v(eight, BF), v(halves, BF),
        v(users, BF), v(chunks, BF), v(users, BF),
        v(plane, BF), v(plane, BF),
        v(halves, BF), v(halves, BF), v(pairs, BF), v(pairs, BF),
        v((2, HIDP, ALL), F32),
        v((2, 2, 2 * SHARE + 16, 128), BF), v((2, 2, 2 * SHARE + 16, 128), BF),
        v((2, HIDP, 128), BF),
        v((PK, 128), F32),
        v((128, PK, 128), BF),
        sem((11,)), sem((5,)), sem((5, 2, LINE)), sem((5,)), sem((5, 2)), sem((5, 2, LINE)), sem((2, 2, 3)),
    ]
    any_space = pl.BlockSpec(memory_space=pl.ANY)
    attended, layer = pl.pallas_call(
        kernel,
        out_shape=(jax.ShapeDtypeStruct((COL, TOK), F32), jax.ShapeDtypeStruct((COL, TOK), F32)),
        in_specs=[any_space] * 11,
        out_specs=(pl.BlockSpec(memory_space=pltpu.VMEM), pl.BlockSpec(memory_space=pltpu.VMEM)),
        scratch_shapes=scratch,
        compiler_params=pltpu.CompilerParams(
            collective_id=0, has_side_effects=True, vmem_limit_bytes=66700000
        ),
        name="layer",
    )(
        tokens, gain_attn.reshape(D // 128, 128), w_query.T, query_bias.reshape(1, COL), cache_keys, cache_values,
        w_out.T, gain_ffn.reshape(1, COL), w_gate.T, w_up.T, w_down,
    )
    return attended.T.astype(BF), layer.T.astype(BF)


def solution(mesh):
    placed = (
        P("mp", None), P(), P(None, "seq"), P("seq"), P(None, "seq", None), P(None, "seq", None),
        P(None, "seq"), P("seq"), P("mp", "seq"), P("mp", "seq"), P("seq", "mp"),
    )
    return jax.shard_map(
        body, mesh=mesh, in_specs=placed, out_specs=(P("mp", "seq"), P("mp", "seq")), check_vma=False
    )
```

```python
import functools
import math

import jax
import jax.numpy as jnp
from jax import lax
from jax.experimental import pallas as pl
from jax.experimental.pallas import tpu as pltpu
from jax.sharding import PartitionSpec as P

D = 3584
HEAD = 128
GROUP = 7
KV = 4
CTX = 1024
SEQ = 64
MP = 4
TOK = 64
ALL = TOK * MP
COL = 56
FEAT = D // MP
PEER = FEAT // COL
HID = 296
SHARE = 160
HIDP = 2 * SHARE
PK = 32
LINE = 8
EPS = 1e-06
MESH = pl.DeviceIdType.MESH
BF = jnp.bfloat16
F32 = jnp.float32
LOG2E = 1.0 / math.log(2.0)


def dot(a, b, dims=((1,), (0,))):
    return lax.dot_general(a, b, (dims, ((), ())), preferred_element_type=F32)


def low_lanes(rows):
    return lax.broadcasted_iota(jnp.int32, (rows, 128), 1) < 64


def row_ids(rows):
    return lax.broadcasted_iota(jnp.int32, (rows, 128), 0)


def swap(x):
    return pltpu.roll(x, 64, axis=1)


def column_of(row):
    n = row.shape[1]
    same = lax.broadcasted_iota(jnp.int32, (n, n), 0) == lax.broadcasted_iota(jnp.int32, (n, n), 1)
    return jnp.sum(jnp.where(same, jnp.broadcast_to(row, (n, n)), 0.0), axis=1, keepdims=True)


def split3(x):
    first = x.astype(BF).astype(F32)
    rest = x - first
    second = rest.astype(BF).astype(F32)
    return first, second, rest - second


def three_rows(x, rows, base=0):
    first, second, third = split3(x)
    at = lax.broadcasted_iota(jnp.int32, (rows, x.shape[1]), 0) - base
    return jnp.where(at == 0, first, jnp.where(at == 1, second, jnp.where(at == 2, third, 0.0)))


def merge(chunks, j):
    at = row_ids(8)
    high = jnp.logical_not(low_lanes(chunks.shape[0]))
    sides = ([], [])
    for i in range(chunks.shape[0]):
        part = chunks[i, 24:PK]
        sides[0].append(jnp.sum(jnp.where(at < 3, part, 0.0), axis=0, keepdims=True))
        sides[1].append(jnp.sum(jnp.where(jnp.logical_and(at >= 3, at < 6), part, 0.0), axis=0, keepdims=True))
    weights, levels = [], []
    for rows in sides:
        level = jnp.concatenate(rows, axis=0)
        level = jnp.where(high, level, swap(level))
        top = jnp.max(level, axis=0, keepdims=True)
        weight = jnp.exp2(level - top)
        total = jnp.sum(weight, axis=0, keepdims=True)
        weights.append(weight / total)
        levels.append(top + jnp.log(total) * LOG2E)
    edge = HEAD * ((j * COL) // HEAD + 1) - j * COL
    first_head = row_ids(PK) + jnp.where(low_lanes(PK), 0, PK) < edge
    acc = jnp.zeros((PK, 128), F32)
    for i in range(chunks.shape[0]):
        acc += chunks[i] * jnp.where(first_head, weights[0][i : i + 1], weights[1][i : i + 1])
    return acc, levels


def kernel(
    tokens_h, gain_attn_h, wq_h, bias_h, keys_h, values_h, wo_h, gain_ffn_h, wg_h, wu_h, wd_h,
    att_out, lay_out,
    tokens, gain_attn, wq, bias, keys, values, wo, gain_ffn, wg, wu, wd,
    normed, value_t, wd_t, hid_t, wo_e, work, outs, lsplit, stage2, stage6,
    own1, own4, held1, line3, held4, buf1, buf3, buf4, plane2, plane6, rel2, rel6, held2, held6,
    gu, gstage, gbuf, act, res, many,
    in_sem, zsend, zrecv, psend, precv, rrecv, asem,
):
    s = lax.axis_index("seq")
    m = lax.axis_index("mp")
    z, x, yh = lax.rem(s, LINE), lax.rem(s // LINE, 4), s // (4 * LINE)
    yl, c = m // 2, lax.rem(m, 2)
    line = s - z
    here = s // LINE
    xb = lax.rem(x, 2)
    own_j = LINE * xb + z
    mine = x // 2 == c
    same_y = yl == yh
    here_y = jnp.logical_and(same_y, yl == c)

    bar = pltpu.get_barrier_semaphore()

    def greet(p, q):
        pl.semaphore_signal(bar, inc=1, device_id=(p, q), device_id_type=MESH)

    for d in (4, 3, 5, 2, 6, 1, 7, 0):
        for u, v in ((1, 0), (1, 1), (0, 1), (0, 0)):
            for w in range(2):
                if d or u or v or w:
                    p = 32 * lax.rem(yh + u, 2) + LINE * x + lax.rem(z + d, LINE)
                    greet(p, 2 * lax.rem(yl + v, 2) + lax.rem(c + w, 2))
    for i in (2, 1, 3):
        for u in (1, 0):
            for w in range(2):
                p = 32 * lax.rem(yh + u, 2) + LINE * lax.rem(x + i, 4) + z
                greet(p, 2 * yl + lax.rem(c + w, 2))

    pairs = (
        (tokens_h, tokens), (gain_attn_h, gain_attn), (wq_h, wq), (bias_h, bias),
        (keys_h.at[m], keys), (values_h.at[m], values), (wo_h, wo), (gain_ffn_h, gain_ffn),
        (wg_h, wg), (wu_h, wu), (wd_h, wd.at[pl.ds(0, HID)]),
    )
    loads = [pltpu.make_async_copy(a, b, in_sem.at[i]) for i, (a, b) in enumerate(pairs)]
    for load in loads:
        load.start()

    loads[0].wait()
    loads[1].wait()
    normed[pl.ds(TOK, TOK), :] = jnp.zeros((TOK, D), BF)
    gain_row = jnp.concatenate([gain_attn[i : i + 1, :] for i in range(D // 128)], axis=1)

    def norm_rows(i, c):
        at = pl.multiple_of(i * 16, 16)
        x = tokens[pl.ds(at, 16), :].astype(F32)
        mean_sq = jnp.sum(x * x, axis=1, keepdims=True) * (1.0 / D)
        normed[pl.ds(at, 16), :] = (x * lax.rsqrt(mean_sq + EPS) * gain_row).astype(BF)
        return c

    lax.fori_loop(0, TOK // 16, norm_rows, 0)
    loads[2].wait()
    loads[3].wait()
    q_t = dot(wq[...], normed[...], ((1,), (1,))) + column_of(bias[...])
    low32 = low_lanes(PK)

    def packed(x):
        hi = jnp.concatenate([x[PK:COL], jnp.zeros((8, 128), F32)], axis=0)
        return jnp.where(low32, x[0:PK], swap(hi))

    def remote(src, dst, send_sem, recv_sem, p, q):
        pltpu.make_async_remote_copy(
            src_ref=src, dst_ref=dst, send_sem=send_sem, recv_sem=recv_sem, device_id=(p, q), device_id_type=MESH
        ).start()

    def copy(src, dst, send_sem, recv_sem, p, q, local):
        @pl.when(local)
        def _():
            pltpu.make_async_copy(src, dst, recv_sem).start()

        @pl.when(jnp.logical_not(local))
        def _():
            remote(src, dst, send_sem, recv_sem, p, q)

    def arrived(buf, sem):
        pltpu.make_async_copy(buf, buf, sem).wait()

    def near_first(i):
        return lax.rem(jnp.where(lax.rem(i, 2) == 1, (i + 1) // 2, LINE - i // 2), LINE)

    def far_first(i):
        return lax.rem(LINE + LINE // 2 + jnp.where(lax.rem(i, 2) == 1, -((i + 1) // 2), i // 2), LINE)

    def spread_yz(own, held, k):
        for d in (4, 3, 5, 2, 6, 1, 7, 0):
            for u in range(2):
                to = (32 * u + LINE * x + lax.rem(z + d, LINE), 2 * yh + yl)
                sems = (zsend.at[k], zrecv.at[k, 0, (LINE - d) % LINE])
                slot = held.at[z, c]
                if d:
                    remote(own, slot, *sems, *to)
                else:
                    copy(own, slot, *sems, *to, jnp.logical_and(yh == u, here_y))

    def spread_x(held, buf, k):
        def step(i, carry):
            e = near_first(i)
            at = lax.rem(z + e, LINE)
            arrived(held.at[at], zrecv.at[k, 0, e])
            for o in (2, 1, 3, 0):
                to = (32 * yh + LINE * lax.rem(x + o, 4) + z, 2 * yl + x // 2)
                args = (held.at[at], buf.at[c, xb, at], psend.at[k], precv.at[k, c], *to)
                if o:
                    remote(*args)
                else:
                    copy(*args, mine)
            return carry

        lax.fori_loop(0, LINE, step, 0)

    def along_line(held, k):
        for d in (4, 3, 5, 2, 6, 1, 7):
            remote(held.at[z], held.at[z], zsend.at[k], zrecv.at[k, 0, LINE - d], line + lax.rem(z + d, LINE), m)

    def on_to_plane(held, buf, k):
        def step(i, carry):
            e = near_first(i)
            at = lax.rem(z + e, LINE)

            @pl.when(i > 0)
            def _():
                arrived(held.at[at], zrecv.at[k, 0, e])

            for d in range(1, 8):
                p = LINE * lax.rem(here + d, 8) + z
                remote(held.at[at], buf.at[here, at], psend.at[k], precv.at[k, 0], p, m)
            pltpu.make_async_copy(held.at[at], buf.at[here, at], precv.at[k, 0]).start()
            return carry

        lax.fori_loop(0, LINE, step, 0)

    own1[...] = packed(q_t).astype(BF)

    loads[5].wait()
    value_t[...] = values[...].T
    first = lax.broadcasted_iota(jnp.int32, (COL, D), 1) - lax.broadcasted_iota(jnp.int32, (COL, D), 0)
    pick = jnp.where(first == s * COL, 1.0, 0.0).astype(BF)
    normed[pl.ds(0, TOK), :] = tokens[...]
    hid_t[...] = dot(pick, normed[...], ((1,), (1,)))
    loads[10].wait()
    wd[pl.ds(HID, HIDP - HID), :] = jnp.zeros((HIDP - HID, FEAT), BF)
    wd_t[...] = wd[...].T
    outs[pl.ds(FEAT, 8), :] = jnp.zeros((8, ALL), F32)
    gu[:, pl.ds(HID, HIDP - HID), :] = jnp.zeros((2, HIDP - HID, ALL), F32)
    wide = PEER * PK
    c_at = lax.broadcasted_iota(jnp.int32, (FEAT, wide), 1)
    r_at = lax.broadcasted_iota(jnp.int32, (FEAT, wide), 0) - COL * (c_at // PK)
    c_at = lax.rem(c_at, PK)
    pick_lo = jnp.where(r_at == c_at, 1.0, 0.0).astype(BF)
    pick_hi = jnp.where(jnp.logical_and(r_at == c_at + PK, c_at < COL - PK), 1.0, 0.0).astype(BF)
    wo_e[...] = jnp.zeros((128, SEQ * PK), BF)
    loads[6].wait()
    for i in range(MP):
        part = wo[:, pl.ds(i * FEAT, FEAT)]
        wo_e[pl.ds(0, COL), pl.ds(i * wide, wide)] = dot(part, pick_lo).astype(BF)
        wo_e[pl.ds(64, COL), pl.ds(i * wide, wide)] = dot(part, pick_hi).astype(BF)
    for i in (4, 7, 8, 9):
        loads[i].wait()

    pl.semaphore_wait(bar, 75)
    spread_yz(own1, held1, 0)
    spread_x(held1, buf1, 0)

    def unpack_chunks(buf, t, squares):
        tile = pl.ds(128 * t, 128)

        def one(j, total):
            a = buf[t, j // LINE, lax.rem(j, LINE), 0].astype(F32)
            b = buf[t, j // LINE, lax.rem(j, LINE), 1].astype(F32)
            lo = jnp.where(low32, a, swap(b))
            hi = jnp.where(low32, swap(a), b)
            at = pl.multiple_of(j * COL, 8)
            work[pl.ds(at, PK), tile] = lo
            work[pl.ds(pl.multiple_of(at + PK, 8), COL - PK), tile] = hi[0 : COL - PK]
            return total + hi[COL - PK : PK] if squares else total

        return lax.fori_loop(0, PEER, one, jnp.zeros((8, 128), F32), unroll=4)

    low8 = low_lanes(8)

    def collect_x(stage, plane, k, t, halves, stats):
        tile = pl.ds(128 * t, 128)

        def step(i, carry):
            e = far_first(i)
            to_z = lax.rem(z + e, LINE)
            for half in halves:
                j = half * LINE + to_z
                r = outs[pl.ds(pl.multiple_of(j * COL, 8), 2 * PK), tile]
                lo, hi = r[0:PK], r[PK : 2 * PK]
                a = jnp.where(low32, lo, swap(hi))
                b = jnp.where(low32, swap(lo), hi)
                if stats:
                    h0, h1 = (j * COL) // HEAD, (j * COL + COL - 1) // HEAD
                    both = jnp.where(row_ids(8) < 3, lsplit[h0, :, tile], lsplit[h1, :, tile])
                    a = jnp.concatenate([a[0:24], jnp.where(low8, a[24:PK], swap(both))], axis=0)
                    b = jnp.concatenate([b[0:24], jnp.where(low8, b[24:PK], both)], axis=0)
                stage[t, to_z, half, 0] = a.astype(BF)
                stage[t, to_z, half, 1] = b.astype(BF)
            for half in halves:
                to = (32 * yh + LINE * (2 * c + half) + z, 2 * yl + t)
                local = jnp.logical_and(2 * c + half == x, c == t)
                copy(stage.at[t, to_z, half], plane.at[to_z, x], psend.at[k], rrecv.at[k, 0, e], *to, local)
            return carry

        lax.fori_loop(0, LINE, step, 0)

    def collect_yz(plane, rel, held, k, join):
        def step(i, carry):
            e = far_first(i)
            to_z = lax.rem(z + e, LINE)
            arrived(plane.at[to_z], rrecv.at[k, 0, e])
            for w in range(2):
                rel[to_z, w] = join(plane[to_z, :, w].astype(F32), to_z).astype(BF)
                to = (32 * yl + LINE * x + to_z, 2 * c + w)
                local = jnp.logical_and(jnp.logical_and(here_y, e == 0), c == w)
                copy(rel.at[to_z, w], held.at[2 * z + yh], zsend.at[k], zrecv.at[k, 0, 0], *to, local)
            return carry

        lax.fori_loop(0, LINE, step, 0)
        arrived(held, zrecv.at[k, 0, 0])

    scale = HEAD ** (-0.5) * LOG2E

    def attend(t, h, n):
        tile = pl.ds(128 * t, 128)
        rows = [pl.ds(pl.multiple_of((h + i) * HEAD, HEAD), HEAD) for i in range(n)]
        queries = jnp.concatenate([work[r, tile].astype(BF) for r in rows], axis=1)
        scores = dot(keys[...], queries) * scale
        top = jnp.max(scores, axis=0, keepdims=True)
        probs = jnp.exp2(scores - top)
        total = jnp.sum(probs, axis=0, keepdims=True)
        value = dot(value_t[...], probs.astype(BF)) * (1.0 / total)
        level = top + jnp.log(total) * LOG2E
        parts = three_rows(level, 8) + three_rows(level, 8, 3)
        for i in range(n):
            outs[rows[i], tile] = value[:, 128 * i : 128 * (i + 1)]
            lsplit[h + i, :, tile] = parts[:, 128 * i : 128 * (i + 1)]

    for t in range(2):
        arrived(buf1.at[t], precv.at[0, t])
        unpack_chunks(buf1, t, False)

        def two_heads(i, carry, t=t):
            attend(t, 2 * i, 2)
            return carry

        lax.fori_loop(0, GROUP // 2, two_heads, 0)
        attend(t, GROUP - 1, 1)
        collect_x(stage2, plane2, 1, t, (0, 1), True)

    def join2(chunks, to_z):
        value, levels = merge(chunks, LINE * xb + to_z)
        rows = three_rows(levels[0], 8) + three_rows(levels[1], 8, 3)
        return jnp.concatenate([value[0:24], jnp.where(low8, value[24:PK], rows)], axis=0)

    collect_yz(plane2, rel2, held2, 1, join2)
    merged = merge(held2[...].astype(F32), own_j)[0].astype(BF)
    line3[z] = merged

    along_line(line3, 2)
    on_to_plane(line3, buf3, 2)

    def unpacked(x, out):
        out[pl.ds(0, PK), :] = x[:, 0:64]
        out[pl.ds(PK, COL - PK), :] = swap(x)[0 : COL - PK, 0:64]

    unpacked(merged.astype(F32), att_out)
    res_hid = packed(hid_t[...])
    gain_col = jnp.broadcast_to(column_of(gain_ffn[...]), (COL, 128))
    gain_pk = packed(gain_col)
    arrived(buf3, precv.at[2, 0])
    both = dot(wo_e[...], buf3[...].reshape(SEQ * PK, 128))
    residual = res_hid + packed(both[0:COL] + swap(both[64 : 64 + COL]))
    res[...] = residual

    real = jnp.logical_or(low32, row_ids(PK) < COL - PK)
    squares = jnp.sum(jnp.where(real, residual * residual, 0.0), axis=0, keepdims=True)
    squares = squares + swap(squares)
    scaled = residual * gain_pk
    own4[...] = jnp.where(real, scaled, three_rows(squares, PK, 24)).astype(BF)
    spread_yz(own4, held4, 3)
    spread_x(held4, buf4, 3)

    def rows_of(core):
        return pl.ds(pl.multiple_of(core * SHARE, 16), SHARE)

    def put_sums(ref, gate, up, sq):
        ref[pl.ds(0, SHARE)] = gate.astype(BF)
        ref[pl.ds(SHARE, SHARE)] = up.astype(BF)
        ref[pl.ds(2 * SHARE, 16)] = three_rows(sq, 16).astype(BF)

    def add_sums(ref, gate, up, sq):
        gate = gate + ref[pl.ds(0, SHARE)].astype(F32)
        up = up + ref[pl.ds(SHARE, SHARE)].astype(F32)
        return gate, up, sq + jnp.sum(ref[pl.ds(2 * SHARE, 16)].astype(F32), axis=0, keepdims=True)

    sqs = []
    for t in range(2):
        tile = pl.ds(128 * t, 128)
        arrived(buf4.at[t], precv.at[3, t])
        sq = jnp.sum(unpack_chunks(buf4, t, True), axis=0, keepdims=True)
        features = work[pl.ds(0, FEAT), tile].astype(BF)
        gu[0, pl.ds(0, HID), tile] = dot(wg[...], features)
        gu[1, pl.ds(0, HID), tile] = dot(wu[...], features)
        put_sums(gstage.at[t, 0], gu[0, rows_of(1 - c), tile], gu[1, rows_of(1 - c), tile], sq)
        remote(gstage.at[t, 0], gbuf.at[t, 0], asem.at[0, t, 0], asem.at[1, t, 0], s, 2 * yl + 1 - c)
        sqs.append(sq)
    sums = []
    for t in range(2):
        tile = pl.ds(128 * t, 128)
        arrived(gbuf.at[t, 0], asem.at[1, t, 0])
        gate, up, sq = add_sums(gbuf.at[t, 0], gu[0, rows_of(c), tile], gu[1, rows_of(c), tile], sqs[t])
        put_sums(gstage.at[t, 1], gate, up, sq)
        remote(gstage.at[t, 1], gbuf.at[t, 1], asem.at[0, t, 1], asem.at[1, t, 1], s, 2 * (1 - yl) + c)
        sums.append((gate, up, sq))
    for t in range(2):
        arrived(gbuf.at[t, 1], asem.at[1, t, 1])
        gate, up, sq = add_sums(gbuf.at[t, 1], *sums[t])
        factor = lax.rsqrt(sq * (1.0 / D) + EPS)
        gate = gate * factor
        up = up * factor
        act[t, rows_of(c)] = (gate / (1.0 + jnp.exp(-gate)) * up).astype(BF)
        part = act.at[t, rows_of(c)]
        remote(part, part, asem.at[0, t, 2], asem.at[1, t, 2], s, 2 * yl + 1 - c)

    for t in range(2):
        arrived(act.at[t, rows_of(1 - c)], asem.at[1, t, 2])
        outs[pl.ds(0, FEAT), pl.ds(128 * t, 128)] = dot(wd_t[...], act[t])
        collect_x(stage6, plane6, 4, t, (0, 1), False)
    collect_yz(plane6, rel6, held6, 4, lambda chunks, to_z: jnp.sum(chunks, axis=0))
    unpacked(res[...] + jnp.sum(held6[...].astype(F32), axis=0), lay_out)

    def sent(cases, sem):
        for holds, n in cases:

            @pl.when(holds)
            def _(n=n):
                arrived(many.at[pl.ds(0, n)], sem)

    for k in (0, 1, 3, 4):
        sent(((here_y, 15), (jnp.logical_not(here_y), 16)), zsend.at[k])
        sent(((mine, 48), (jnp.logical_not(mine), 64)), psend.at[k])
    arrived(many.at[pl.ds(0, 7)], zsend.at[2])
    arrived(many.at[pl.ds(0, 56)], psend.at[2])
    for t in range(2):
        arrived(gstage.at[t, 0], asem.at[0, t, 0])
        arrived(gstage.at[t, 1], asem.at[0, t, 1])
        arrived(act.at[t, rows_of(c)], asem.at[0, t, 2])


def body(tokens, gain_attn, w_query, query_bias, cache_keys, cache_values, w_out, gain_ffn, w_gate, w_up, w_down):
    v = pltpu.VMEM
    one, eight, pairs, halves = (PK, 128), (LINE, PK, 128), (2 * LINE, PK, 128), (LINE, 2, PK, 128)
    chunks, users = (8, LINE, PK, 128), (2, 2, LINE, 2, PK, 128)
    owners, plane = (2, LINE, 2, 2, PK, 128), (LINE, 4, 2, PK, 128)
    sem = pltpu.SemaphoreType.DMA
    scratch = [
        v((TOK, D), BF), v((D // 128, 128), F32), v((COL, D), BF), v((1, COL), F32), v((CTX, HEAD), BF),
        v((CTX, HEAD), BF), v((COL, D), BF), v((1, COL), F32), v((HID, FEAT), BF), v((HID, FEAT), BF),
        v((HIDP, FEAT), BF),
        v((2 * TOK, D), BF),
        v((HEAD, CTX), BF),
        v((FEAT, HIDP), BF),
        v((COL, 128), F32),
        v((128, SEQ * PK), BF),
        v((FEAT, ALL), F32),
        v((FEAT + 8, ALL), F32),
        v((8, 8, ALL), F32),
        v(owners, BF), v(owners, BF),
        v(one, BF), v(one, BF), v(halves, BF), v((LINE, PK, 128), BF), v(halves, BF),
        v(users, BF), v(chunks, BF), v(users, BF),
        v(plane, BF), v(plane, BF),
        v(halves, BF), v(halves, BF), v(pairs, BF), v(pairs, BF),
        v((2, HIDP, ALL), F32),
        v((2, 2, 2 * SHARE + 16, 128), BF), v((2, 2, 2 * SHARE + 16, 128), BF),
        v((2, HIDP, 128), BF),
        v((PK, 128), F32),
        v((64, PK, 128), BF),
        sem((11,)), sem((5,)), sem((5, 2, LINE)), sem((5,)), sem((5, 2)), sem((5, 2, LINE)), sem((2, 2, 3)),
    ]
    any_space = pl.BlockSpec(memory_space=pl.ANY)
    attended, layer = pl.pallas_call(
        kernel,
        out_shape=(jax.ShapeDtypeStruct((COL, TOK), F32), jax.ShapeDtypeStruct((COL, TOK), F32)),
        in_specs=[any_space] * 11,
        out_specs=(pl.BlockSpec(memory_space=pltpu.VMEM), pl.BlockSpec(memory_space=pltpu.VMEM)),
        scratch_shapes=scratch,
        compiler_params=pltpu.CompilerParams(
            collective_id=0, has_side_effects=True, vmem_limit_bytes=66700000
        ),
        name="layer",
    )(
        tokens, gain_attn.reshape(D // 128, 128), w_query.T, query_bias.reshape(1, COL), cache_keys, cache_values,
        w_out.T, gain_ffn.reshape(1, COL), w_gate.T, w_up.T, w_down,
    )
    return attended.T.astype(BF), layer.T.astype(BF)


def solution(mesh):
    placed = (
        P("mp", None), P(), P(None, "seq"), P("seq"), P(None, "seq", None), P(None, "seq", None),
        P(None, "seq"), P("seq"), P("mp", "seq"), P("mp", "seq"), P("seq", "mp"),
    )
    return jax.shard_map(
        body, mesh=mesh, in_specs=placed, out_specs=(P("mp", "seq"), P("mp", "seq")), check_vma=False
    )
```
